128 devices in a mesh: row: 16 (over y_lo, z, core), col: 8 (over x, y_hi).
Axes of the slice: x: 4, y: 4 (y_hi: 2, y_lo: 2; y = y_hi * 2 + y_lo), z: 4, core: 2. Of those that a mesh axis runs over, the one named last changes fastest.
Arguments:
- potential: float32 [512, 512, 512], P(('row', 'col')), may hold values from -6 to 6
- basis_left: bfloat16 [8192, 128, 384], P(('row', 'col')), may hold values from -1.1953125 to 1.1953125
- basis_right: bfloat16 [8192, 128, 384], P(('row', 'col')), may hold values from -1.1953125 to 1.1953125
- core_matrix: bfloat16 [8192, 8192], P('row', 'col'), may hold values from -3 to 3
- density: bfloat16 [8192, 8192], P('row', 'col'), as said below
- pattern: int32 [64, 64], replicated, may hold values from 0 to 1, as said below
- pair_atoms: int32 [8192, 2], P(('row', 'col')), may hold values from 0 to 63, as said below
- cube_offsets: int32 [8192, 3], P(('row', 'col')), may hold values from 0 to 504, as said below
- live_count: int32 [128], P(('row', 'col')), may hold values from 32 to 64, as said below
Outputs:
- hamiltonian: bfloat16 [8192, 8192], P('row', 'col')
- product: float32 [8192, 8192], P('row', 'col')
The draws below stay inside these ranges and needn't reach their ends.
Inputs may be any that keep to these rules, and one draw needn't show every extreme that they name: `pattern`: symmetric; every diagonal block is 1. density is symmetric. `pair_atoms`: the owner of block (i, j) is (i // 4, j // 8) on a 16 x 8 grid. Among the 64 entry slots of one slab at most 1 name blocks of one owner, and in every draw one owner is named by a live entry of every slab. `cube_offsets`: column 0 is at most 2, column 1 at most 504, column 2 at most 504. `live_count`: some slab uses all its slots.
All inputs are finite; a program needn't handle non-finite values.
Results may differ from the reference program's by a relative error of at most 0.0092.
Values may be sent and summed in bfloat16 or wider, within the bound.
No kernel may reach another device: no remote copies, remote signals or barrier semaphores. Data moves between devices by JAX's collectives and lax.ppermute only.
A program may use at most 192 MiB of HBM per device.

```python
import math
import jax
import jax.numpy as jnp
from jax import lax

NB = 128
NATOMS = 64
CX = 4
NY = 512
NZ = 512
E_DEV = 64
HALO = 2
CUBE_X = 6
CUBE = 8
CUBE_CELLS = 384
NBAS = 8192
NX = 512
SLOTS = 8192
N_ROW = 16
N_COL = 8


def broad_shift(key):
    return jax.random.randint(jax.random.fold_in(key, 41), (), 0, NATOMS // N_COL).astype(jnp.int32)


def draw_density(key, part):
    order = NATOMS * NB
    base_key = jax.random.fold_in(key, 5)
    base = jax.random.normal(base_key, (order, order), jnp.float32)
    return ((base + base.T) * (0.70710678 / math.sqrt(order))).astype(jnp.bfloat16)


def draw_pattern(key, part):
    col_atoms = NATOMS // N_COL
    reach = jax.random.randint(jax.random.fold_in(key, 3), (NATOMS,), 1, NATOMS // 4 + 1)
    index = jnp.arange(NATOMS, dtype=jnp.int32)
    reach = jnp.where(index % col_atoms == broad_shift(key), NATOMS // 2, reach)
    apart = jnp.abs(index[:, None] - index[None, :])
    apart = jnp.minimum(apart, NATOMS - apart)
    return (apart <= jnp.maximum(reach[:, None], reach[None, :])).astype(jnp.int32)


def draw_pair_atoms(key, part):
    devices = N_ROW * N_COL
    capacity = (E_DEV + devices - 1) // devices
    hot_owner = jax.random.randint(jax.random.fold_in(key, 7), (), 0, devices)
    slab_keys = jax.random.split(jax.random.fold_in(key, 9), devices)

    def slab_order(slab_key):
        others = capacity + jax.random.permutation(slab_key, devices * capacity - capacity)
        joined = jnp.concatenate([jnp.arange(capacity, dtype=jnp.int32), others.astype(jnp.int32)])
        return joined[:E_DEV]
    orders = jax.vmap(slab_order)(slab_keys)
    owners = (orders + hot_owner * capacity) % (devices * capacity) // capacity
    row_atoms = NATOMS // N_ROW
    col_atoms = NATOMS // N_COL
    local_block = jax.random.randint(jax.random.fold_in(key, 11), (devices, E_DEV), 0, row_atoms * col_atoms)
    first_atom = owners // N_COL * row_atoms + local_block // col_atoms
    second_atom = owners % N_COL * col_atoms + local_block % col_atoms
    slot_index = jnp.arange(E_DEV, dtype=jnp.int32)[None, :]
    broad_atom = owners % N_COL * col_atoms + broad_shift(key)
    second_atom = jnp.where(slot_index < 2, broad_atom, second_atom)
    return jnp.stack([first_atom, second_atom], axis=-1).reshape(devices * E_DEV, 2).astype(jnp.int32)


def draw_cube_offsets(key, part):
    total = N_ROW * N_COL * E_DEV
    top_x = CX + 2 * HALO - CUBE_X
    slot_index = jnp.arange(total, dtype=jnp.int32) % E_DEV
    along_x = jax.random.randint(jax.random.fold_in(key, 19), (total,), 0, top_x + 1)
    along_x = jnp.where(slot_index == 0, 0, jnp.where(slot_index == 1, top_x, along_x))
    along_y = jax.random.randint(jax.random.fold_in(key, 23), (total,), 0, NY - CUBE + 1)
    along_z = jax.random.randint(jax.random.fold_in(key, 29), (total,), 0, NZ - CUBE + 1)
    return jnp.stack([along_x, along_y, along_z], axis=-1).astype(jnp.int32)


def draw_live_count(key, part):
    devices = N_ROW * N_COL
    counts = jax.random.randint(jax.random.fold_in(key, 13), (devices,), E_DEV // 2, E_DEV + 1)
    fullest = jax.random.randint(jax.random.fold_in(key, 17), (), 0, devices)
    return jnp.where(jnp.arange(devices) == fullest, E_DEV, counts).astype(jnp.int32)


def shard_levels(key, dims, cuts, smallest, largest):
    factor_of = 1.0
    for axis_at, parts in cuts:
        heights = jax.random.uniform(jax.random.fold_in(jax.random.fold_in(key, 6), axis_at), (parts,), jnp.float32, smallest / len(cuts), largest / len(cuts))
        factor_of = factor_of * jnp.repeat(jnp.exp(heights), dims[axis_at] // parts).reshape((-1,) + (1,) * (len(dims) - 1 - axis_at))
    return factor_of


def bell_draw(stream_key, shape, deviation, bound, cuts=(), kind=jnp.bfloat16):
    entries = deviation * jax.random.normal(stream_key, shape, jnp.float32)
    if cuts:
        entries = entries * shard_levels(stream_key, shape, cuts, -0.22, 0.18)
    return jnp.clip(entries, -bound, bound).astype(kind)


def setup_inputs(seed: int = 0) -> dict:
    key_list = jax.random.split(jax.random.key(seed), 10)
    return {
        "potential": bell_draw(key_list[0], (NX, NY, NZ), 1.0, 6.0, ((0, 128),), jnp.float32),
        "basis_left": bell_draw(key_list[1], (SLOTS, NB, CUBE_CELLS), 0.2, 1.1953125, ((0, 128),)),
        "basis_right": bell_draw(key_list[2], (SLOTS, NB, CUBE_CELLS), 0.2, 1.1953125, ((0, 128),)),
        "core_matrix": bell_draw(key_list[3], (NBAS, NBAS), 0.5, 3.0, ((0, 16), (1, 8))),
        "density": draw_density(jax.random.fold_in(key_list[9], 71), 0),
        "pattern": draw_pattern(jax.random.fold_in(key_list[9], 71), 0),
        "pair_atoms": draw_pair_atoms(jax.random.fold_in(key_list[9], 71), 0),
        "cube_offsets": draw_cube_offsets(jax.random.fold_in(key_list[9], 71), 0),
        "live_count": draw_live_count(jax.random.fold_in(key_list[9], 71), 0),
    }


HIGHEST = lax.Precision.HIGHEST


def block_mask(values, pattern_tile, block_size):
    row_blocks, col_blocks = pattern_tile.shape
    shaped = values.reshape(row_blocks, block_size, col_blocks, block_size)
    selected = (pattern_tile > 0)[:, None, :, None]
    kept = jnp.where(selected, shaped, jnp.zeros((), values.dtype))
    return kept.reshape(row_blocks * block_size, col_blocks * block_size)


def reference(potential, basis_left, basis_right, core_matrix, density, pattern, pair_atoms, cube_offsets, live_count):
    devices = N_ROW * N_COL
    slab_planes = NX // devices
    slot_total = pair_atoms.shape[0]
    per_slab = slot_total // devices
    ordinal = jnp.arange(slot_total, dtype=jnp.int32)
    slab_index = ordinal // per_slab
    live_flag = ((ordinal % per_slab) < live_count[slab_index]).astype(jnp.float32)

    def integrate(entry):
        left_table, right_table, offsets, slab_number, flag_value = entry
        planes = (slab_number * slab_planes - HALO + offsets[0] + jnp.arange(CUBE_X, dtype=jnp.int32)) % NX
        slab_rows = jnp.take(potential, planes.astype(jnp.int32), axis=0)
        start = (jnp.zeros((), jnp.int32), offsets[1].astype(jnp.int32), offsets[2].astype(jnp.int32))
        cube_cells = lax.dynamic_slice(slab_rows, start, (CUBE_X, CUBE, CUBE)).reshape(-1)
        weighted = (left_table.astype(jnp.float32) * cube_cells[None, :]).astype(jnp.bfloat16)
        block_value = jnp.dot(weighted.astype(jnp.float32), right_table.astype(jnp.float32).T, precision=HIGHEST)
        return block_value * flag_value

    partials = lax.map(integrate, (basis_left, basis_right, cube_offsets, slab_index, live_flag))
    block_id = (pair_atoms[:, 0] * NATOMS + pair_atoms[:, 1]).astype(jnp.int32)
    summed = jax.ops.segment_sum(partials, block_id, num_segments=NATOMS * NATOMS)
    integrals = summed.reshape(NATOMS, NATOMS, NB, NB).transpose(0, 2, 1, 3).reshape(NATOMS * NB, NATOMS * NB)
    hamiltonian = block_mask(core_matrix.astype(jnp.float32) + integrals, pattern, NB).astype(jnp.bfloat16)
    masked_density = block_mask(density, pattern, NB)
    product = jnp.dot(hamiltonian.astype(jnp.float32), masked_density.astype(jnp.float32), precision=HIGHEST)
    return hamiltonian, product
```

```python
import functools

import jax
import jax.numpy as jnp
from jax import lax
from jax.experimental import pallas as pl
from jax.experimental.pallas import tpu as pltpu
from jax.sharding import Mesh
from jax.sharding import PartitionSpec as P

NATOMS = 64
NB = 128
ENTRIES = 64
DEVICES = 128
ATOM_ROWS = 4
ATOM_COLS = 8
CELLS = 384
ROW = ("yl", "z", "c")
COL = ("x", "yh")
ALL = ("yl", "z", "c", "x", "yh")


SMEM = pl.BlockSpec(memory_space=pltpu.SMEM)


def shift(array, axis, step):
    size = lax.axis_size(axis)
    return lax.ppermute(array, axis, [(i, (i + step) % size) for i in range(size)])


def cut_pair(slab, first_plane, y0, z0):
    tile = z0 // 128
    within = z0 - tile * 128
    tile_after = jnp.minimum(tile + 1, 3)
    lane = lax.broadcasted_iota(jnp.int32, (8, 128), 1)
    sub = lax.broadcasted_iota(jnp.int32, (8, 128), 0)
    from_low = (lane % 64) + within < 128
    planes = []
    for k in range(2):
        turn = (128 + 64 * k - within) % 128
        plane = 2048 * (first_plane + k) + y0
        here = pltpu.roll(slab[pl.ds(plane + 512 * tile, 8), :], turn, 1)
        after = pltpu.roll(slab[pl.ds(plane + 512 * tile_after, 8), :], turn, 1)
        planes.append(jnp.where(from_low, here, after))
    both = jnp.where(lane < 64, planes[0], planes[1])
    for bit in range(3):
        both = jnp.where((sub >> bit) & 1 == 1, pltpu.roll(both, 8 << bit, 1), both)
    both = jnp.where((lane // 8) % 8 == sub, both, 0.0)
    return jnp.sum(both, axis=0, keepdims=True)


def edge_kernel(prev_ref, next_ref, slab, prev_out, next_out):
    @pl.loop(0, ENTRIES, unroll=4)
    def _(e):
        prev_out[pl.ds(e, 1), :] = cut_pair(slab, 0, prev_ref[e], prev_ref[ENTRIES + e])
        next_out[pl.ds(e, 1), :] = cut_pair(slab, 2, next_ref[e], next_ref[ENTRIES + e])


def own_kernel(own_ref, slab, out):
    @pl.loop(0, ENTRIES, unroll=4)
    def _(e):
        for k in range(2):
            out[k, pl.ds(e, 1), :] = cut_pair(
                slab, 2 * k, own_ref[e], own_ref[ENTRIES + e]
            )


def cut_edges(prev_yz, next_yz, potential):
    shape = jax.ShapeDtypeStruct((ENTRIES, 128), jnp.float32)
    return pl.pallas_call(
        edge_kernel,
        out_shape=(shape, shape),
        in_specs=[SMEM, SMEM, pl.BlockSpec(memory_space=pltpu.VMEM)],
        name="cut_edges",
    )(prev_yz, next_yz, potential)


def cut_own(yz, potential):
    return pl.pallas_call(
        own_kernel,
        out_shape=jax.ShapeDtypeStruct((2, ENTRIES, 128), jnp.float32),
        in_specs=[SMEM, pl.BlockSpec(memory_space=pltpu.VMEM)],
        name="cut_own",
    )(yz, potential)


GROUP = 8


def partial_kernel(owner_ref, live_ref, cubes, left, right, out):
    step = pl.program_id(0)

    @pl.when(step == 0)
    def _():
        out[...] = jnp.zeros_like(out)

    for g in range(GROUP):
        e = step * GROUP + g

        @pl.when(e < live_ref[0])
        def _():
            cube = cubes[pl.ds(g, 1), :]
            weighted = (left[g].astype(jnp.float32) * cube).astype(jnp.bfloat16)
            block = lax.dot_general(
                weighted, right[g], (((1,), (1,)), ((), ())), preferred_element_type=jnp.float32
            )
            out[owner_ref[e]] = block.astype(jnp.bfloat16)


def partial_blocks(owner, live, cubes, left, right):
    return pl.pallas_call(
        partial_kernel,
        grid_spec=pltpu.PrefetchScalarGridSpec(
            num_scalar_prefetch=2,
            grid=(ENTRIES // GROUP,),
            in_specs=[
                pl.BlockSpec((GROUP, CELLS), lambda i, *_: (i, 0)),
                pl.BlockSpec((GROUP, NB, CELLS), lambda i, *_: (i, 0, 0)),
                pl.BlockSpec((GROUP, NB, CELLS), lambda i, *_: (i, 0, 0)),
            ],
            out_specs=pl.BlockSpec((DEVICES, NB, NB), lambda i, *_: (0, 0, 0)),
        ),
        out_shape=jax.ShapeDtypeStruct((DEVICES, NB, NB), jnp.bfloat16),
        name="partial_blocks",
    )(owner, live, cubes, left, right)


SUM_GROUP = 16


def sum_kernel(ids_ref, pattern_ref, core, received, full, top, bottom, total):
    step = pl.program_id(0)

    @pl.when(step == 0)
    def _():
        total[...] = core[...].astype(jnp.float32)

    for g in range(SUM_GROUP):
        mark = ids_ref[step * SUM_GROUP + g]

        @pl.when(mark > 0)
        def _():
            where = mark - 1
            rows = pl.ds(pl.multiple_of(where // ATOM_COLS * NB, NB), NB)
            cols = pl.ds(pl.multiple_of(where % ATOM_COLS * NB, NB), NB)
            total[rows, cols] += received[g].astype(jnp.float32)

    @pl.when(step == pl.num_programs(0) - 1)
    def _():
        for i in range(ATOM_ROWS):
            for j in range(ATOM_COLS):
                block = total[i * NB : i * NB + NB, j * NB : j * NB + NB]
                keep = pattern_ref[i * ATOM_COLS + j] > 0
                block = jnp.where(keep, block, 0.0).astype(jnp.bfloat16)
                full[i * NB : i * NB + NB, j * NB : j * NB + NB] = block
                half = top if i < 2 else bottom
                half[(i % 2) * NB : (i % 2) * NB + NB, j * NB : j * NB + NB] = block


def hamiltonian_tile(ids, pattern_tile, core, received):
    rows, cols = core.shape
    whole = lambda i, *_: (0, 0)
    return pl.pallas_call(
        sum_kernel,
        grid_spec=pltpu.PrefetchScalarGridSpec(
            num_scalar_prefetch=2,
            grid=(DEVICES // SUM_GROUP,),
            in_specs=[
                pl.BlockSpec((rows, cols), whole),
                pl.BlockSpec((SUM_GROUP, NB, NB), lambda i, *_: (i, 0, 0)),
            ],
            out_specs=[
                pl.BlockSpec((rows, cols), whole),
                pl.BlockSpec((rows // 2, cols), whole),
                pl.BlockSpec((rows // 2, cols), whole),
            ],
            scratch_shapes=[pltpu.VMEM((rows, cols), jnp.float32)],
        ),
        out_shape=(
            jax.ShapeDtypeStruct((rows, cols), jnp.bfloat16),
            jax.ShapeDtypeStruct((rows // 2, cols), jnp.bfloat16),
            jax.ShapeDtypeStruct((rows // 2, cols), jnp.bfloat16),
        ),
        name="sum_blocks",
    )(ids, pattern_tile, core, received)


def product_kernel(count, has_acc, slot_ref, core_ref, *refs):
    pieces = refs[:count]
    own_a, other_a, own_b, other_b = refs[count : count + 4]
    acc = refs[count + 4] if has_acc else None
    out = refs[-1]
    step = pl.program_id(0)
    c = core_ref[0]

    @pl.when(step == 0)
    def _():
        if has_acc:
            out[...] = acc[...]
        else:
            out[...] = jnp.zeros_like(out)

    for k in range(count):

        @pl.when(step == k)
        def _(k=k):
            mine = pieces[k][:, pl.ds(pl.multiple_of(c * 512, 512), 512)]
            theirs = pieces[k][:, pl.ds(pl.multiple_of((1 - c) * 512, 512), 512)]
            for half, (own, other) in enumerate(((own_a, other_a), (own_b, other_b))):
                cols = slice(half * 512, half * 512 + 512)
                out[:, cols] += jnp.dot(
                    mine, own[0], preferred_element_type=jnp.float32
                ) + jnp.dot(theirs, other[0], preferred_element_type=jnp.float32)


def multiply(acc, pieces, slots, core, density):
    count = len(pieces)
    rows, cols = pieces[0].shape
    whole = lambda i, *_: (0, 0)
    picked = pl.BlockSpec((1, 512, 512), lambda i, slot, c: (slot[i], 0, 0))
    shape = jax.ShapeDtypeStruct((rows, 1024), jnp.float32)
    has_acc = acc is not None
    return pl.pallas_call(
        functools.partial(product_kernel, count, has_acc),
        grid_spec=pltpu.PrefetchScalarGridSpec(
            num_scalar_prefetch=2,
            grid=(count,),
            in_specs=[pl.BlockSpec((rows, cols), whole)] * count
            + [picked] * 4
            + [pl.BlockSpec((rows, 1024), whole)] * has_acc,
            out_specs=pl.BlockSpec((rows, 1024), whole),
        ),
        out_shape=shape,
        name="product",
    )(slots, core, *pieces, *density, *([acc] if has_acc else []))


def after(value, *others):
    return lax.optimization_barrier((value,) + others)[0]


def block_mask(values, pattern_tile, block_size):
    row_blocks, col_blocks = pattern_tile.shape
    shaped = values.reshape(row_blocks, block_size, col_blocks, block_size)
    selected = (pattern_tile > 0)[:, None, :, None]
    kept = jnp.where(selected, shaped, jnp.zeros((), values.dtype))
    return kept.reshape(row_blocks * block_size, col_blocks * block_size)


def shards(
    potential,
    basis_left,
    basis_right,
    core_matrix,
    density,
    pattern,
    pair_atoms,
    cube_offsets,
    live_count,
):
    x, yh = lax.axis_index("x"), lax.axis_index("yh")
    yl, z, c = lax.axis_index("yl"), lax.axis_index("z"), lax.axis_index("c")

    yz = jnp.concatenate([cube_offsets[:, 1], cube_offsets[:, 2]])
    prev_yz = shift(yz, ALL, 1)
    next_yz = shift(yz, ALL, -1)

    corner = (lax.axis_index(ROW) * ATOM_ROWS, lax.axis_index(COL) * ATOM_COLS)
    pattern_tile = lax.dynamic_slice(pattern, corner, (ATOM_ROWS, ATOM_COLS))
    masked = block_mask(density, pattern_tile, NB)
    da, db = masked[:, :512], masked[:, 512:]
    da_y = shift(da, "yl", 1)
    db_p, db_m = shift(db, "z", 1), shift(db, "z", -1)

    ordinal = jnp.arange(ENTRIES, dtype=jnp.int32)
    first, second = pair_atoms[:, 0], pair_atoms[:, 1]
    owner = first // ATOM_ROWS * 8 + second // ATOM_COLS
    local = first % ATOM_ROWS * ATOM_COLS + second % ATOM_COLS
    sent = (owner[None, :] == jnp.arange(DEVICES, dtype=jnp.int32)[:, None]) & (
        ordinal < live_count[0]
    )[None, :]
    marks = jnp.sum(jnp.where(sent, local[None, :] + 1, 0), axis=1)
    marks = lax.all_to_all(marks, ALL, 0, 0, tiled=True)

    columns = potential.reshape(4, 512, 4, 128).transpose(0, 2, 1, 3).reshape(8192, 128)
    for_prev, for_next = cut_edges(prev_yz, next_yz, columns)
    high = shift(for_prev, ALL, -1)
    low = shift(for_next, ALL, 1)
    own = cut_own(yz, columns)
    extended = jnp.concatenate([low, own[0], own[1], high], axis=1)
    along = cube_offsets[:, :1]
    cubes = jnp.where(
        along == 0,
        extended[:, :384],
        jnp.where(along == 1, extended[:, 64:448], extended[:, 128:]),
    )
    outgoing = partial_blocks(owner, live_count, cubes, basis_left, basis_right)
    received = lax.all_to_all(outgoing, ALL, 0, 0, tiled=True)

    db_o1, db_o2 = shift(db_p[:256], "z", 1), shift(db_m[256:], "z", -1)
    da_p, day_p = shift(da, "z", 1), shift(da_y, "z", 1)
    da_m, day_m = shift(da, "z", -1), shift(da_y, "z", -1)
    da_o, day_o = shift(da_p, "z", 1), shift(day_m, "z", -1)
    db_o = jnp.concatenate([db_o1, db_o2])
    dby, dby_p, dby_m, dby_o = (shift(v, "yl", 1) for v in (db, db_p, db_m, db_o))
    own_a = jnp.stack([da, da_p, da_o, da_m, da_y, day_p, day_o, day_m])
    own_b = jnp.stack([db, db_p, db_o, db_m, dby, dby_p, dby_o, dby_m])
    other_a, other_b = shift(own_a, "c", 1), shift(own_b, "c", 1)
    density_slots = (own_a, other_a, own_b, other_b)

    hamiltonian, ha, hb = hamiltonian_tile(marks, pattern_tile.reshape(-1), core_matrix, received)

    ha_y = shift(ha, "yh", 1)
    hb_p, hb_m = shift(hb, "x", 1), shift(hb, "x", -1)
    ha_p, ha_m = shift(ha, "x", 1), shift(ha, "x", -1)
    hby = shift(hb, "yh", 1)
    hay_p, hay_m = shift(ha_y, "x", 1), shift(ha_y, "x", -1)
    hb_o1, hb_o2 = shift(hb_p[:128], "x", 1), shift(hb_m[128:], "x", -1)
    hby_p, hby_m = shift(hb_p, "yh", 1), shift(hb_m, "yh", 1)
    ha_o, hay_o = shift(ha_p, "x", 1), shift(hay_m, "x", -1)
    hb_o = jnp.concatenate([hb_o1, hb_o2])
    hby_o = shift(hb_o, "yh", 1)

    def slot_of(dx, dy):
        block = (x - dx) % 4 * 2 + (yh + dy) % 2
        far, plane = block // 4, block % 4
        return ((far - yl) % 2) * 4 + (z - plane) % 4

    def slots(*relative):
        return jnp.stack([slot_of(dx, dy) for dx, dy in relative]).astype(jnp.int32)

    core = c.reshape(1).astype(jnp.int32)
    top = multiply(None, [ha, ha_y, ha_p, ha_m], slots((0, 0), (0, 1), (1, 0), (-1, 0)), core, density_slots)
    bottom = multiply(None, [hb, hby, hb_p, hb_m], slots((0, 0), (0, 1), (1, 0), (-1, 0)), core, density_slots)
    top = multiply(top, [hay_p, hay_m, ha_o, hay_o], slots((1, 1), (-1, 1), (2, 0), (2, 1)), core, density_slots)
    bottom = multiply(bottom, [hby_p, hby_m, hb_o, hby_o], slots((1, 1), (-1, 1), (2, 0), (2, 1)), core, density_slots)
    return hamiltonian, jnp.concatenate([top, bottom])


def solution(mesh):
    split = Mesh(mesh.devices.reshape(2, 4, 2, 4, 2), ALL)
    placed = (
        P(ALL, None, None),
        P(ALL, None, None),
        P(ALL, None, None),
        P(ROW, COL),
        P(ROW, COL),
        P(),
        P(ALL, None),
        P(ALL, None),
        P(ALL),
    )
    return jax.shard_map(
        shards,
        mesh=split,
        in_specs=placed,
        out_specs=(P(ROW, COL), P(ROW, COL)),
        check_vma=False,
    )
```

```python
import functools

import jax
import jax.numpy as jnp
from jax import lax
from jax.experimental import pallas as pl
from jax.experimental.pallas import tpu as pltpu
from jax.sharding import Mesh
from jax.sharding import PartitionSpec as P


NB = 128
ENTRIES = 64
DEVICES = 128
ATOM_ROWS = 4
ATOM_COLS = 8
CELLS = 384
ROW = ("yl", "z", "c")
COL = ("x", "yh")
ALL = ("yl", "z", "c", "x", "yh")


SMEM = pl.BlockSpec(memory_space=pltpu.SMEM)


def shift(array, axis, step):
    size = lax.axis_size(axis)
    return lax.ppermute(array, axis, [(i, (i + step) % size) for i in range(size)])


def turned_pair(slab, first_plane, y0, z0):
    tile = z0 >> 7
    within = z0 & 127
    tile_after = jnp.minimum(tile + 1, 3)
    lane = lax.broadcasted_iota(jnp.int32, (8, 128), 1)
    from_low = (lane & 63) + within < 128
    planes = []
    for k in range(2):
        turn = (128 + 64 * k - within) & 127
        plane = 2048 * (first_plane + k) + y0
        here = pltpu.roll(slab[pl.ds(plane + 512 * tile, 8), :], turn, 1)
        after = pltpu.roll(slab[pl.ds(plane + 512 * tile_after, 8), :], turn, 1)
        planes.append(jnp.where(from_low, here, after))
    return jnp.where(lane < 64, planes[0], planes[1])


def as_rows(windows):
    lane = lax.broadcasted_iota(jnp.int32, windows.shape, 1)
    sub = lax.broadcasted_iota(jnp.int32, windows.shape, 0) & 7
    for bit in range(3):
        windows = jnp.where((sub >> bit) & 1 == 1, pltpu.roll(windows, 8 << bit, 1), windows)
    windows = jnp.where((lane >> 3) & 7 == sub, windows, 0.0)
    return jnp.sum(windows.reshape(-1, 8, 128), axis=1)


def load_columns(potential, slab, sem):
    copies = [
        pltpu.make_async_copy(
            potential.at[p, :, 128 * t : 128 * t + 128],
            slab.at[(p * 4 + t) * 512 : (p * 4 + t) * 512 + 512, :],
            sem.at[p * 4 + t],
        )
        for p in range(4)
        for t in range(4)
    ]
    for copy in copies:
        copy.start()
    for copy in copies:
        copy.wait()


def edge_kernel(prev_ref, next_ref, potential, prev_out, next_out, slab, held, sem):
    load_columns(potential, slab, sem)

    @pl.loop(0, ENTRIES, unroll=8)
    def _(e):
        row = pl.multiple_of(e * 8, 8)
        held[0, pl.ds(row, 8), :] = turned_pair(slab, 0, prev_ref[e], prev_ref[ENTRIES + e])
        held[1, pl.ds(row, 8), :] = turned_pair(slab, 2, next_ref[e], next_ref[ENTRIES + e])

    prev_out[...] = as_rows(held[0])
    next_out[...] = as_rows(held[1])


def own_kernel(own_ref, potential, out, slab, held, sem):
    load_columns(potential, slab, sem)

    @pl.loop(0, ENTRIES, unroll=8)
    def _(e):
        row = pl.multiple_of(e * 8, 8)
        for k in range(2):
            held[k, pl.ds(row, 8), :] = turned_pair(slab, 2 * k, own_ref[e], own_ref[ENTRIES + e])

    for k in range(2):
        out[k] = as_rows(held[k])


CUT_SCRATCH = [
    pltpu.VMEM((16 * 512, 128), jnp.float32),
    pltpu.VMEM((2, ENTRIES * 8, 128), jnp.float32),
    pltpu.SemaphoreType.DMA((16,)),
]


def cut_edges(prev_yz, next_yz, potential):
    shape = jax.ShapeDtypeStruct((ENTRIES, 128), jnp.float32)
    return pl.pallas_call(
        edge_kernel,
        out_shape=(shape, shape),
        in_specs=[SMEM, SMEM, pl.BlockSpec(memory_space=pl.ANY)],
        scratch_shapes=CUT_SCRATCH,
        name="cut_edges",
    )(prev_yz, next_yz, potential)


def cut_own(yz, potential):
    return pl.pallas_call(
        own_kernel,
        out_shape=jax.ShapeDtypeStruct((2, ENTRIES, 128), jnp.float32),
        in_specs=[SMEM, pl.BlockSpec(memory_space=pl.ANY)],
        scratch_shapes=CUT_SCRATCH,
        name="cut_own",
    )(yz, potential)


GROUP = 8


TAIL = 8


def partial_kernel(owner_ref, mark_ref, cubes, left, right, out):
    step = pl.program_id(0)

    @pl.when(step == 0)
    def _():
        out[:, NB:, :] = jnp.zeros((DEVICES, TAIL, NB), jnp.bfloat16)

    for g in range(GROUP):
        e = step * GROUP + g
        weighted = (left[g].astype(jnp.float32) * cubes[g : g + 1, :]).astype(jnp.bfloat16)
        block = lax.dot_general(
            weighted, right[g], (((1,), (1,)), ((), ())), preferred_element_type=jnp.float32
        )
        owner = owner_ref[e]
        out[owner, :NB, :] = block.astype(jnp.bfloat16)
        out[owner, NB:, :] = jnp.full((TAIL, NB), mark_ref[e].astype(jnp.float32)).astype(
            jnp.bfloat16
        )


def partial_blocks(owner, mark, cubes, left, right):
    return pl.pallas_call(
        partial_kernel,
        grid_spec=pltpu.PrefetchScalarGridSpec(
            num_scalar_prefetch=2,
            grid=(ENTRIES // GROUP,),
            in_specs=[
                pl.BlockSpec((GROUP, CELLS), lambda i, *_: (i, 0)),
                pl.BlockSpec((GROUP, NB, CELLS), lambda i, *_: (i, 0, 0)),
                pl.BlockSpec((GROUP, NB, CELLS), lambda i, *_: (i, 0, 0)),
            ],
            out_specs=pl.BlockSpec((DEVICES, NB + TAIL, NB), lambda i, *_: (0, 0, 0)),
        ),
        out_shape=jax.ShapeDtypeStruct((DEVICES, NB + TAIL, NB), jnp.bfloat16),
        name="partial_blocks",
    )(owner, mark, cubes, left, right)


SUM_GROUP = 16


def sum_kernel(pattern_ref, core_ref, core, received, full, mine, theirs, total):
    step = pl.program_id(0)

    @pl.when(step == 0)
    def _():
        total[: ATOM_ROWS * NB, :] = core[...].astype(jnp.float32)

    marks = [
        jnp.max(received[g, NB:, :].astype(jnp.float32)).astype(jnp.int32)
        for g in range(SUM_GROUP)
    ]
    for g, mark in enumerate(marks):
        where = jnp.where(mark > 0, mark - 1, ATOM_ROWS * ATOM_COLS)
        rows = pl.ds(pl.multiple_of((where >> 3) * NB, NB), NB)
        cols = pl.ds(pl.multiple_of((where & 7) * NB, NB), NB)
        total[rows, cols] += received[g, :NB, :].astype(jnp.float32)

    @pl.when(step == pl.num_programs(0) - 1)
    def _():
        c = core_ref[0]
        for i in range(ATOM_ROWS):
            rows = slice(i * NB, i * NB + NB)
            for j in range(ATOM_COLS):
                cols = slice(j * NB, j * NB + NB)
                keep = pattern_ref[i * ATOM_COLS + j] > 0
                full[rows, cols] = jnp.where(keep, total[rows, cols], 0.0).astype(jnp.bfloat16)
        mine[...] = full[:, pl.ds(pl.multiple_of(c * 512, 512), 512)]
        theirs[...] = full[:, pl.ds(pl.multiple_of((1 - c) * 512, 512), 512)]


def hamiltonian_tile(pattern_tile, core_index, core, received):
    rows, cols = core.shape
    whole = lambda i, *_: (0, 0)
    half = pl.BlockSpec((rows, cols // 2), whole)
    half_shape = jax.ShapeDtypeStruct((rows, cols // 2), jnp.bfloat16)
    return pl.pallas_call(
        sum_kernel,
        grid_spec=pltpu.PrefetchScalarGridSpec(
            num_scalar_prefetch=2,
            grid=(DEVICES // SUM_GROUP,),
            in_specs=[
                pl.BlockSpec((rows, cols), whole),
                pl.BlockSpec((SUM_GROUP, NB + TAIL, NB), lambda i, *_: (i, 0, 0)),
            ],
            out_specs=[pl.BlockSpec((rows, cols), whole), half, half],
            scratch_shapes=[pltpu.VMEM((rows + NB, cols), jnp.float32)],
        ),
        out_shape=(jax.ShapeDtypeStruct((rows, cols), jnp.bfloat16), half_shape, half_shape),
        name="sum_blocks",
    )(pattern_tile, core_index, core, received)


def product_kernel(work, has_acc, place, *refs):
    count = len(work)
    pieces, tiles = refs[:count], refs[count : count + 4]
    acc = refs[count + 4] if has_acc else None
    out, columns, rows, column_sem, row_sem = refs[-5:]
    x, yh, yl, z, way = (place[i] for i in range(5))

    for k, (side, steps, turn) in enumerate(work):
        pltpu.make_async_copy(pieces[k], columns.at[k], column_sem.at[k]).start()
        block = ((x - way * steps) & 3) * 2 + ((yh + turn) & 1)
        plane = ((way if side == "own" else -way) * (z - block)) & 3
        far = ((block >> 2) + yl) & 1
        base = 0 if side == "own" else 2
        for which in range(2):

            @pl.when(far == which)
            def _(k=k, base=base, which=which, plane=plane):
                pltpu.make_async_copy(
                    tiles[base + which].at[plane], rows.at[k], row_sem.at[k]
                ).start()

    out[...] = acc[...] if has_acc else jnp.zeros_like(out)

    @pl.loop(0, count)
    def _(k):
        pltpu.make_async_copy(pieces[0], columns.at[k], column_sem.at[k]).wait()
        pltpu.make_async_copy(tiles[0].at[0], rows.at[k], row_sem.at[k]).wait()
        out[...] += jnp.dot(columns[k], rows[k], preferred_element_type=jnp.float32)


def multiply(place, acc, work, density):
    pieces = [w[3] for w in work]
    count = len(work)
    work = tuple(w[:3] for w in work)
    given = [] if acc is None else [acc]
    vmem = pl.BlockSpec(memory_space=pltpu.VMEM)
    return pl.pallas_call(
        functools.partial(product_kernel, work, acc is not None),
        in_specs=[SMEM] + [pl.BlockSpec(memory_space=pl.ANY)] * (count + 4) + [vmem] * len(given),
        out_specs=vmem,
        scratch_shapes=[
            pltpu.VMEM((count, 512, 512), jnp.bfloat16),
            pltpu.VMEM((count, 512, 1024), jnp.bfloat16),
            pltpu.SemaphoreType.DMA((count,)),
            pltpu.SemaphoreType.DMA((count,)),
        ],
        out_shape=jax.ShapeDtypeStruct((512, 1024), jnp.float32),
        name="product",
    )(place, *pieces, *density, *given)


def block_mask(values, pattern_tile, block_size):
    row_blocks, col_blocks = pattern_tile.shape
    shaped = values.reshape(row_blocks, block_size, col_blocks, block_size)
    selected = (pattern_tile > 0)[:, None, :, None]
    kept = jnp.where(selected, shaped, jnp.zeros((), values.dtype))
    return kept.reshape(row_blocks * block_size, col_blocks * block_size)


def turn(array, axis, step):
    axes = ("z", "c") if axis == "z" else ("c", "x")
    pairs = []
    for c in range(2):
        for i in range(4):
            to = (i + (step if c == 0 else -step)) % 4
            pairs.append((i * 2 + c, to * 2 + c) if axis == "z" else (c * 4 + i, c * 4 + to))
    return lax.ppermute(array, axes, pairs)


def steps(
    potential, basis_left, basis_right, core_matrix, density, pattern, pair_atoms, cube_offsets,
    live_count,
):
    x, yh = lax.axis_index("x"), lax.axis_index("yh")
    yl, z, c = lax.axis_index("yl"), lax.axis_index("z"), lax.axis_index("c")

    yz = jnp.concatenate([cube_offsets[:, 1], cube_offsets[:, 2]])
    prev_yz = shift(yz, ALL, 1)
    next_yz = shift(yz, ALL, -1)

    corner = (lax.axis_index(ROW) * ATOM_ROWS, lax.axis_index(COL) * ATOM_COLS)
    pattern_tile = lax.dynamic_slice(pattern, corner, (ATOM_ROWS, ATOM_COLS))
    d = block_mask(density, pattern_tile, NB)
    dy = shift(d, "yl", 1)
    d_1, d_2 = turn(d, "z", 1), turn(d, "z", -1)

    for_prev, for_next = cut_edges(prev_yz, next_yz, potential)
    high = shift(for_prev, ALL, -1)
    low = shift(for_next, ALL, 1)
    own = cut_own(yz, potential)
    extended = jnp.concatenate([low, own[0], own[1], high], axis=1)
    along = cube_offsets[:, :1]
    cubes = jnp.where(
        along == 0,
        extended[:, :384],
        jnp.where(along == 1, extended[:, 64:448], extended[:, 128:]),
    )

    ordinal = jnp.arange(ENTRIES, dtype=jnp.int32)
    first, second = pair_atoms[:, 0], pair_atoms[:, 1]
    owner = first // ATOM_ROWS * 8 + second // ATOM_COLS
    local = first % ATOM_ROWS * ATOM_COLS + second % ATOM_COLS
    mark = jnp.where(ordinal < live_count[0], local + 1, 0)
    outgoing = partial_blocks(owner, mark, cubes, basis_left, basis_right)
    received = lax.all_to_all(outgoing, ALL, 0, 0, tiled=True)

    d_o = turn(d_1, "z", 1)
    dy_1, dy_2 = turn(dy, "z", 1), turn(dy, "z", -1)
    near = jnp.stack([d, d_1, d_o, d_2])
    near_other = shift(near, "c", 1)
    core_index = c.reshape(1).astype(jnp.int32)
    hamiltonian, ha, hb = hamiltonian_tile(
        pattern_tile.reshape(-1), core_index, core_matrix, received
    )
    dy_o = turn(dy_1, "z", 1)
    away = jnp.stack([dy, dy_1, dy_o, dy_2])
    away_other = shift(away, "c", 1)
    tiles = (near, away, near_other, away_other)

    hb_1, hb_2 = turn(hb, "x", 1), turn(hb, "x", -1)
    ha_y = shift(ha, "yh", 1)
    ha_1, ha_2 = turn(ha, "x", 1), turn(ha, "x", -1)
    hb_y = shift(hb, "yh", 1)
    hb_o = turn(hb_1, "x", 1)
    hb_y1, hb_y2 = shift(hb_1, "yh", 1), shift(hb_2, "yh", 1)
    ha_y1, ha_y2 = turn(ha_y, "x", 1), turn(ha_y, "x", -1)
    ha_o = turn(ha_1, "x", 1)
    hb_yo = shift(hb_o, "yh", 1)
    ha_yo = turn(ha_y1, "x", 1)

    place = jnp.stack([x, yh, yl, z, 1 - 2 * c]).astype(jnp.int32)
    out = multiply(
        place,
        None,
        [
            ("own", 0, 0, ha),
            ("other", 0, 0, hb),
            ("other", 1, 0, hb_1),
            ("other", -1, 0, hb_2),
            ("own", 0, 1, ha_y),
            ("own", 1, 0, ha_1),
            ("own", -1, 0, ha_2),
            ("other", 0, 1, hb_y),
        ],
        tiles,
    )
    out = multiply(
        place,
        out,
        [
            ("other", 2, 0, hb_o),
            ("own", 1, 1, ha_y1),
            ("own", -1, 1, ha_y2),
            ("own", 2, 0, ha_o),
            ("other", 1, 1, hb_y1),
            ("other", -1, 1, hb_y2),
        ],
        tiles,
    )
    out = multiply(
        place, out, [("own", 2, 1, ha_yo), ("other", 2, 1, hb_yo)], tiles
    )
    return hamiltonian, out


def solution(mesh):
    split = Mesh(mesh.devices.reshape(2, 4, 2, 4, 2), ALL)
    placed = (
        P(ALL, None, None),
        P(ALL, None, None),
        P(ALL, None, None),
        P(ROW, COL),
        P(ROW, COL),
        P(),
        P(ALL, None),
        P(ALL, None),
        P(ALL),
    )
    return jax.shard_map(
        steps,
        mesh=split,
        in_specs=placed,
        out_specs=(P(ROW, COL), P(ROW, COL)),
        check_vma=False,
    )
```

```python
import functools

import jax
import jax.numpy as jnp
from jax import lax
from jax.experimental import pallas as pl
from jax.experimental.pallas import tpu as pltpu
from jax.sharding import Mesh
from jax.sharding import PartitionSpec as P


NB = 128
ENTRIES = 64
DEVICES = 128
ATOM_ROWS = 4
ATOM_COLS = 8
CELLS = 384
ROW = ("yl", "z", "c")
COL = ("x", "yh")
ALL = ("yl", "z", "c", "x", "yh")


SMEM = pl.BlockSpec(memory_space=pltpu.SMEM)


def shift(array, axis, step):
    size = lax.axis_size(axis)
    return lax.ppermute(array, axis, [(i, (i + step) % size) for i in range(size)])


def turned_pair(slab, first_plane, y0, z0):
    tile = z0 >> 7
    within = z0 & 127
    tile_after = jnp.minimum(tile + 1, 3)
    lane = lax.broadcasted_iota(jnp.int32, (8, 128), 1)
    planes = []
    for k in range(2):
        plane = 2048 * (first_plane + k) + y0
        here = slab[pl.ds(plane + 512 * tile, 8), :]
        after = slab[pl.ds(plane + 512 * tile_after, 8), :]
        turn = (128 + 64 * k - within) & 127
        planes.append(pltpu.roll(jnp.where(lane >= within, here, after), turn, 1))
    return jnp.where(lane < 64, planes[0], planes[1])


def as_rows(windows):
    lane = lax.broadcasted_iota(jnp.int32, windows.shape, 1)
    sub = lax.broadcasted_iota(jnp.int32, windows.shape, 0) & 7
    for bit in range(3):
        windows = jnp.where((sub >> bit) & 1 == 1, pltpu.roll(windows, 8 << bit, 1), windows)
    windows = jnp.where((lane >> 3) & 7 == sub, windows, 0.0)
    return jnp.sum(windows.reshape(-1, 8, 128), axis=1)


def load_columns(potential, slab, sem):
    copies = [
        pltpu.make_async_copy(
            potential.at[p, :, 128 * t : 128 * t + 128],
            slab.at[(p * 4 + t) * 512 : (p * 4 + t) * 512 + 512, :],
            sem.at[p * 4 + t],
        )
        for p in range(4)
        for t in range(4)
    ]
    for copy in copies:
        copy.start()
    for copy in copies:
        copy.wait()


def edge_kernel(prev_ref, next_ref, potential, prev_out, next_out, slab, held, sem):
    load_columns(potential, slab, sem)

    @pl.loop(0, ENTRIES, unroll=8)
    def _(e):
        row = pl.multiple_of(e * 8, 8)
        held[0, pl.ds(row, 8), :] = turned_pair(slab, 0, prev_ref[1, e], prev_ref[2, e])
        held[1, pl.ds(row, 8), :] = turned_pair(slab, 2, next_ref[1, e], next_ref[2, e])

    prev_out[...] = as_rows(held[0])
    next_out[...] = as_rows(held[1])


def own_kernel(own_ref, potential, out, slab, held, sem):
    load_columns(potential, slab, sem)

    @pl.loop(0, ENTRIES, unroll=8)
    def _(e):
        row = pl.multiple_of(e * 8, 8)
        for k in range(2):
            held[k, pl.ds(row, 8), :] = turned_pair(slab, 2 * k, own_ref[1, e], own_ref[2, e])

    for k in range(2):
        out[k] = as_rows(held[k])


CUT_SCRATCH = [
    pltpu.VMEM((16 * 512, 128), jnp.float32),
    pltpu.VMEM((2, ENTRIES * 8, 128), jnp.float32),
    pltpu.SemaphoreType.DMA((16,)),
]


def cut_edges(prev_offsets, next_offsets, potential):
    shape = jax.ShapeDtypeStruct((ENTRIES, 128), jnp.float32)
    return pl.pallas_call(
        edge_kernel,
        out_shape=(shape, shape),
        in_specs=[SMEM, SMEM, pl.BlockSpec(memory_space=pl.ANY)],
        scratch_shapes=CUT_SCRATCH,
        name="cut_edges",
    )(prev_offsets, next_offsets, potential)


def cut_own(offsets, potential):
    return pl.pallas_call(
        own_kernel,
        out_shape=jax.ShapeDtypeStruct((2, ENTRIES, 128), jnp.float32),
        in_specs=[SMEM, pl.BlockSpec(memory_space=pl.ANY)],
        scratch_shapes=CUT_SCRATCH,
        name="cut_own",
    )(offsets, potential)


GROUP = 8


TAIL = 8


def partial_kernel(pair_ref, live_ref, cubes, left, right, out):
    step = pl.program_id(0)

    @pl.when(step == 0)
    def _():
        out[:, NB:, :] = jnp.zeros((DEVICES, TAIL, NB), jnp.bfloat16)

    for g in range(GROUP):
        e = step * GROUP + g
        weighted = (left[g].astype(jnp.float32) * cubes[g : g + 1, :]).astype(jnp.bfloat16)
        block = lax.dot_general(
            weighted, right[g], (((1,), (1,)), ((), ())), preferred_element_type=jnp.float32
        )
        first, second = pair_ref[0, e], pair_ref[1, e]
        owner = (first >> 2) * 8 + (second >> 3)
        mark = jnp.where(e < live_ref[0], (first & 3) * ATOM_COLS + (second & 7) + 1, 0)
        out[owner, :NB, :] = block.astype(jnp.bfloat16)
        out[owner, NB:, :] = jnp.full((TAIL, NB), mark.astype(jnp.float32)).astype(jnp.bfloat16)


def partial_blocks(pairs, live, cubes, left, right):
    return pl.pallas_call(
        partial_kernel,
        grid_spec=pltpu.PrefetchScalarGridSpec(
            num_scalar_prefetch=2,
            grid=(ENTRIES // GROUP,),
            in_specs=[
                pl.BlockSpec((GROUP, CELLS), lambda i, *_: (i, 0)),
                pl.BlockSpec((GROUP, NB, CELLS), lambda i, *_: (i, 0, 0)),
                pl.BlockSpec((GROUP, NB, CELLS), lambda i, *_: (i, 0, 0)),
            ],
            out_specs=pl.BlockSpec((DEVICES, NB + TAIL, NB), lambda i, *_: (0, 0, 0)),
        ),
        out_shape=jax.ShapeDtypeStruct((DEVICES, NB + TAIL, NB), jnp.bfloat16),
        name="partial_blocks",
    )(pairs, live, cubes, left, right)


SUM_GROUP = 16


def sum_kernel(pattern_ref, core, received, full, even, odd):
    step = pl.program_id(0)
    height = ATOM_ROWS * NB

    @pl.when(step == 0)
    def _():
        even[:height, :] = core[...].astype(jnp.float32)
        odd[...] = jnp.zeros_like(odd)

    marks = [
        received[g, NB:, :].astype(jnp.float32)[0, 0].astype(jnp.int32) for g in range(SUM_GROUP)
    ]
    for g, mark in enumerate(marks):
        where = jnp.where(mark > 0, mark - 1, ATOM_ROWS * ATOM_COLS)
        rows = pl.ds(pl.multiple_of((where >> 3) * NB, NB), NB)
        cols = pl.ds(pl.multiple_of((where & 7) * NB, NB), NB)
        total = even if g % 2 == 0 else odd
        total[rows, cols] += received[g, :NB, :].astype(jnp.float32)

    @pl.when(step == pl.num_programs(0) - 1)
    def _():
        for i in range(ATOM_ROWS):
            rows = slice(i * NB, i * NB + NB)
            for j in range(ATOM_COLS):
                cols = slice(j * NB, j * NB + NB)
                keep = pattern_ref[i * ATOM_COLS + j] > 0
                block = even[rows, cols] + odd[rows, cols]
                full[rows, cols] = jnp.where(keep, block, 0.0).astype(jnp.bfloat16)


def hamiltonian_tile(pattern_tile, core, received):
    rows, cols = core.shape
    whole = pl.BlockSpec((rows, cols), lambda i, *_: (0, 0))
    return pl.pallas_call(
        sum_kernel,
        grid_spec=pltpu.PrefetchScalarGridSpec(
            num_scalar_prefetch=1,
            grid=(DEVICES // SUM_GROUP,),
            in_specs=[
                whole,
                pl.BlockSpec((SUM_GROUP, NB + TAIL, NB), lambda i, *_: (i, 0, 0)),
            ],
            out_specs=whole,
            scratch_shapes=[pltpu.VMEM((rows + NB, cols), jnp.float32)] * 2,
        ),
        out_shape=jax.ShapeDtypeStruct((rows, cols), jnp.bfloat16),
        name="sum_blocks",
    )(pattern_tile, core, received)


def product_kernel(count, first, has_acc, index, *refs):
    pieces, own, other = refs[:count], refs[count], refs[count + 1]
    acc = refs[count + 2] if has_acc else None
    out, columns, rows, column_sem, row_sem = refs[-5:]
    mine = pl.multiple_of(index[0] * 512, 512)
    theirs = pl.multiple_of(512 - index[0] * 512, 512)

    for k in range(count):
        pltpu.make_async_copy(pieces[k], columns.at[k], column_sem.at[k]).start()
        for s, (stack, base, at) in enumerate(((own, 1, mine), (other, 9, theirs))):
            pltpu.make_async_copy(
                stack.at[index[base + first + k]], rows.at[k, pl.ds(at, 512), :], row_sem.at[k, s]
            ).start()

    out[...] = acc[...] if has_acc else jnp.zeros_like(out)

    @pl.loop(0, count)
    def _(k):
        pltpu.make_async_copy(pieces[0], columns.at[k], column_sem.at[k]).wait()
        for s, at in enumerate((mine, theirs)):
            pltpu.make_async_copy(
                own.at[0], rows.at[k, pl.ds(at, 512), :], row_sem.at[k, s]
            ).wait()
        out[...] += jnp.dot(columns[k], rows[k], preferred_element_type=jnp.float32)


def multiply(index, first, acc, pieces, own, other):
    count = len(pieces)
    given = [] if acc is None else [acc]
    vmem = pl.BlockSpec(memory_space=pltpu.VMEM)
    return pl.pallas_call(
        functools.partial(product_kernel, count, first, acc is not None),
        in_specs=[SMEM] + [pl.BlockSpec(memory_space=pl.ANY)] * (count + 2) + [vmem] * len(given),
        out_specs=vmem,
        scratch_shapes=[
            pltpu.VMEM((count, 512, 1024), jnp.bfloat16),
            pltpu.VMEM((count, 1024, 1024), jnp.bfloat16),
            pltpu.SemaphoreType.DMA((count,)),
            pltpu.SemaphoreType.DMA((count, 2)),
        ],
        out_shape=jax.ShapeDtypeStruct((512, 1024), jnp.float32),
        name="product",
    )(index, *pieces, own, other, *given)


def block_mask(values, pattern_tile, block_size):
    row_blocks, col_blocks = pattern_tile.shape
    shaped = values.reshape(row_blocks, block_size, col_blocks, block_size)
    selected = (pattern_tile > 0)[:, None, :, None]
    kept = jnp.where(selected, shaped, jnp.zeros((), values.dtype))
    return kept.reshape(row_blocks * block_size, col_blocks * block_size)


ROUTES = (
    (0, (0, 1), (1, 0)),
    (0, (1, 0), (-1, 0)),
    (0, (-1, 0), (0, 1)),
    (1, (-1, 0), (1, 0)),
    (1, (1, 0), (0, 1)),
    (2, (1, 0), (0, 1)),
    (4, (-1, 0), (0, 1)),
)


def come_from(core):
    found = [(0, 0)]
    for source, *moves in ROUTES:
        steps, cross = moves[core]
        at = found[source]
        found.append(((at[0] - steps) % 4, (at[1] + cross) % 2))
    return found


def tile_at(core):
    found = come_from(core)
    return [found.index((i % 4, i // 4)) for i in range(8)]


def send(array, ring, k):
    _, *moves = ROUTES[k]
    axes = ("yl", "z", "c") if ring == "z" else ("c", "x", "yh")
    pairs = []
    for c in range(2):
        steps, cross = moves[c]
        for i in range(4):
            for y in range(2):
                to_i, to_y = (i + steps) % 4, (y + cross) % 2
                if ring == "z":
                    pairs.append(((y * 4 + i) * 2 + c, (to_y * 4 + to_i) * 2 + c))
                else:
                    pairs.append(((c * 4 + i) * 2 + y, (c * 4 + to_i) * 2 + to_y))
    return lax.ppermute(array, axes, pairs)


def steps(
    potential, basis_left, basis_right, core_matrix, density, pattern, pair_atoms, cube_offsets,
    live_count,
):
    x, yh = lax.axis_index("x"), lax.axis_index("yh")
    yl, z, c = lax.axis_index("yl"), lax.axis_index("z"), lax.axis_index("c")

    offsets = cube_offsets.T
    prev_offsets = shift(offsets, ALL, 1)
    next_offsets = shift(offsets, ALL, -1)

    corner = (lax.axis_index(ROW) * ATOM_ROWS, lax.axis_index(COL) * ATOM_COLS)
    pattern_tile = lax.dynamic_slice(pattern, corner, (ATOM_ROWS, ATOM_COLS))
    d = [block_mask(density, pattern_tile, NB)]
    for k in range(7):
        d.append(send(d[ROUTES[k][0]], "z", k))

    for_prev, for_next = cut_edges(prev_offsets, next_offsets, potential)
    high = shift(for_prev, ALL, -1)
    low = shift(for_next, ALL, 1)
    own = cut_own(offsets, potential)
    extended = jnp.concatenate([low, own[0], own[1], high], axis=1)
    along = cube_offsets[:, :1]
    cubes = jnp.where(
        along == 0,
        extended[:, :384],
        jnp.where(along == 1, extended[:, 64:448], extended[:, 128:]),
    )
    outgoing = partial_blocks(pair_atoms.T, live_count, cubes, basis_left, basis_right)
    received = lax.all_to_all(outgoing, ALL, 0, 0, tiled=True)

    own_rows = jnp.stack(d)
    other_rows = shift(own_rows, "c", 1)

    hamiltonian = hamiltonian_tile(pattern_tile.reshape(-1), core_matrix, received)
    h = [hamiltonian]
    for k in range(7):
        h.append(send(h[ROUTES[k][0]], "x", k))

    sources = jnp.where(c == 0, jnp.array(come_from(0)), jnp.array(come_from(1)))
    block = ((x + sources[:, 0]) & 3) * 2 + ((yh + sources[:, 1]) & 1)
    at = (((block >> 2) + yl) & 1) * 4 + ((block - z) & 3)
    first, second = jnp.array(tile_at(0)), jnp.array(tile_at(1))
    hot = (at[:, None] == jnp.arange(8)[None, :]).astype(jnp.int32)
    in_own = jnp.sum(hot * jnp.where(c == 0, first, second)[None, :], axis=1)
    in_other = jnp.sum(hot * jnp.where(c == 0, second, first)[None, :], axis=1)
    index = jnp.concatenate([c.reshape(1), in_own, in_other]).astype(jnp.int32)

    out = multiply(index, 0, None, h[:4], own_rows, other_rows)
    out = multiply(index, 4, out, h[4:7], own_rows, other_rows)
    out = multiply(index, 7, out, h[7:], own_rows, other_rows)
    return hamiltonian, out


def solution(mesh):
    split = Mesh(mesh.devices.reshape(2, 4, 2, 4, 2), ALL)
    placed = (
        P(ALL, None, None),
        P(ALL, None, None),
        P(ALL, None, None),
        P(ROW, COL),
        P(ROW, COL),
        P(),
        P(ALL, None),
        P(ALL, None),
        P(ALL),
    )
    return jax.shard_map(
        steps,
        mesh=split,
        in_specs=placed,
        out_specs=(P(ROW, COL), P(ROW, COL)),
        check_vma=False,
    )
```

```python
import functools

import jax
import jax.numpy as jnp
from jax import lax
from jax.experimental import pallas as pl
from jax.experimental.pallas import tpu as pltpu
from jax.sharding import Mesh
from jax.sharding import PartitionSpec as P


NB = 128
ENTRIES = 64
DEVICES = 128
ATOM_ROWS = 4
ATOM_COLS = 8
CELLS = 384
ROW = ("yl", "z", "c")
COL = ("x", "yh")
ALL = ("yl", "z", "c", "x", "yh")


SMEM = pl.BlockSpec(memory_space=pltpu.SMEM)


def shift(array, axis, step):
    size = lax.axis_size(axis)
    return lax.ppermute(array, axis, [(i, (i + step) % size) for i in range(size)])


def turned_pair(slab, first_plane, y0, z0):
    tile = z0 >> 7
    within = z0 & 127
    tile_after = jnp.minimum(tile + 1, 3)
    lane = lax.broadcasted_iota(jnp.int32, (8, 128), 1)
    planes = []
    for k in range(2):
        plane = 2048 * (first_plane + k) + y0
        here = slab[pl.ds(plane + 512 * tile, 8), :]
        after = slab[pl.ds(plane + 512 * tile_after, 8), :]
        turn = (128 + 64 * k - within) & 127
        planes.append(pltpu.roll(jnp.where(lane >= within, here, after), turn, 1))
    return jnp.where(lane < 64, planes[0], planes[1])


def as_rows(windows):
    lane = lax.broadcasted_iota(jnp.int32, windows.shape, 1)
    sub = lax.broadcasted_iota(jnp.int32, windows.shape, 0) & 7
    for bit in range(3):
        windows = jnp.where((sub >> bit) & 1 == 1, pltpu.roll(windows, 8 << bit, 1), windows)
    windows = jnp.where((lane >> 3) & 7 == sub, windows, 0.0)
    return jnp.sum(windows.reshape(-1, 8, 128), axis=1)


def column_copies(potential, slab, sem):
    return [
        pltpu.make_async_copy(
            potential.at[p, :, 128 * t : 128 * t + 128],
            slab.at[(p * 4 + t) * 512 : (p * 4 + t) * 512 + 512, :],
            sem.at[p * 4 + t],
        )
        for p in range(4)
        for t in range(4)
    ]


def cut_both(offset_refs, outs, potential, slab, held, sem):
    copies = column_copies(potential, slab, sem)
    for copy in copies:
        copy.start()
    for k in range(2):
        for copy in copies[8 * k : 8 * k + 8]:
            copy.wait()
        offset_ref = offset_refs[k]

        @pl.loop(0, ENTRIES, unroll=8)
        def _(e, k=k, offset_ref=offset_ref):
            row = pl.multiple_of(e * 8, 8)
            held[k, pl.ds(row, 8), :] = turned_pair(
                slab, 2 * k, offset_ref[1, e], offset_ref[2, e]
            )

        outs[k][...] = as_rows(held[k])


def edge_kernel(prev_ref, next_ref, potential, prev_out, next_out, slab, held, sem):
    cut_both((prev_ref, next_ref), (prev_out, next_out), potential, slab, held, sem)


def own_kernel(own_ref, potential, out, slab, held, sem):
    cut_both((own_ref, own_ref), (out.at[0], out.at[1]), potential, slab, held, sem)


CUT_SCRATCH = [
    pltpu.VMEM((16 * 512, 128), jnp.float32),
    pltpu.VMEM((2, ENTRIES * 8, 128), jnp.float32),
    pltpu.SemaphoreType.DMA((16,)),
]


def cut_edges(prev_offsets, next_offsets, potential):
    shape = jax.ShapeDtypeStruct((ENTRIES, 128), jnp.float32)
    return pl.pallas_call(
        edge_kernel,
        out_shape=(shape, shape),
        in_specs=[SMEM, SMEM, pl.BlockSpec(memory_space=pl.ANY)],
        scratch_shapes=CUT_SCRATCH,
        name="cut_edges",
    )(prev_offsets, next_offsets, potential)


def cut_own(offsets, potential):
    return pl.pallas_call(
        own_kernel,
        out_shape=jax.ShapeDtypeStruct((2, ENTRIES, 128), jnp.float32),
        in_specs=[SMEM, pl.BlockSpec(memory_space=pl.ANY)],
        scratch_shapes=CUT_SCRATCH,
        name="cut_own",
    )(offsets, potential)


GROUP = 8
GROUPS = ENTRIES // GROUP
TAIL = 8


def cube_row(windows, along):
    lane = lax.broadcasted_iota(jnp.int32, (1, 128), 1)
    turned = [pltpu.roll(w, 64, 1) for w in windows]
    cells = []
    for i in range(3):
        between = jnp.where(lane < 64, turned[i], turned[i + 1])
        cells.append(
            jnp.where(along == 0, windows[i], jnp.where(along == 1, between, windows[i + 1]))
        )
    return jnp.concatenate(cells, axis=1)


def partial_kernel(
    pair_ref, live_ref, offset_ref, low, own, high, left, right, out,
    lefts, rights, staged, blank, in_sem, out_sem, blank_sem,
):
    def reads(g):
        rows = pl.ds(g * GROUP, GROUP)
        return (
            pltpu.make_async_copy(left.at[rows], lefts.at[rows], in_sem.at[g, 0]),
            pltpu.make_async_copy(right.at[rows], rights.at[rows], in_sem.at[g, 1]),
        )

    for g in range(GROUPS):
        for copy in reads(g):
            copy.start()
    blank[...] = jnp.zeros_like(blank)
    clear = pltpu.make_async_copy(blank, out.at[:, NB:, :], blank_sem)
    clear.start()
    clear.wait()

    @pl.loop(0, GROUPS)
    def _(g):
        for copy in reads(g):
            copy.wait()
        for i in range(GROUP):
            e = g * GROUP + i
            row = pl.ds(e, 1)
            windows = [low[row, :], own[0, row, :], own[1, row, :], high[row, :]]
            cube = cube_row(windows, offset_ref[0, e])
            weighted = (lefts[e].astype(jnp.float32) * cube).astype(jnp.bfloat16)
            block = lax.dot_general(
                weighted, rights[e], (((1,), (1,)), ((), ())), preferred_element_type=jnp.float32
            )
            first, second = pair_ref[0, e], pair_ref[1, e]
            owner = (first >> 2) * 8 + (second >> 3)
            mark = jnp.where(e < live_ref[0], (first & 3) * ATOM_COLS + (second & 7) + 1, 0)
            staged[e, :NB, :] = block.astype(jnp.bfloat16)
            staged[e, NB:, :] = jnp.full((TAIL, NB), mark.astype(jnp.float32)).astype(jnp.bfloat16)
            pltpu.make_async_copy(staged.at[e], out.at[owner], out_sem.at[e]).start()

    @pl.loop(0, ENTRIES)
    def _(e):
        pltpu.make_async_copy(staged.at[e], out.at[0], out_sem.at[e]).wait()


def partial_blocks(pairs, live, offsets, low, own, high, left, right):
    vmem = pl.BlockSpec(memory_space=pltpu.VMEM)
    hbm = pl.BlockSpec(memory_space=pl.ANY)
    return pl.pallas_call(
        partial_kernel,
        in_specs=[SMEM] * 3 + [vmem] * 3 + [hbm] * 2,
        out_specs=hbm,
        scratch_shapes=[
            pltpu.VMEM((ENTRIES, NB, CELLS), jnp.bfloat16),
            pltpu.VMEM((ENTRIES, NB, CELLS), jnp.bfloat16),
            pltpu.VMEM((ENTRIES, NB + TAIL, NB), jnp.bfloat16),
            pltpu.VMEM((DEVICES, TAIL, NB), jnp.bfloat16),
            pltpu.SemaphoreType.DMA((GROUPS, 2)),
            pltpu.SemaphoreType.DMA((ENTRIES,)),
            pltpu.SemaphoreType.DMA,
        ],
        out_shape=jax.ShapeDtypeStruct((DEVICES, NB + TAIL, NB), jnp.bfloat16),
        name="partial_blocks",
    )(pairs, live, offsets, low, own, high, left, right)


SUM_GROUP = 16
SUM_GROUPS = DEVICES // SUM_GROUP


def sum_kernel(pattern_ref, core, received, full, tile, slots, even, odd, core_sem, slot_sem):
    def read(g):
        rows = pl.ds(g * SUM_GROUP, SUM_GROUP)
        return pltpu.make_async_copy(received.at[rows], slots.at[rows], slot_sem.at[g])

    load = pltpu.make_async_copy(core, tile, core_sem)
    load.start()
    for g in range(SUM_GROUPS):
        read(g).start()
    odd[...] = jnp.zeros_like(odd)
    load.wait()
    for i in range(ATOM_ROWS):
        for j in range(ATOM_COLS):
            block = tile[i * NB : i * NB + NB, j * NB : j * NB + NB]
            even[i * ATOM_COLS + j + 1] = block.astype(jnp.float32)

    @pl.loop(0, SUM_GROUPS)
    def _(g):
        read(g).wait()
        at = [g * SUM_GROUP + i for i in range(SUM_GROUP)]
        marks = [slots[s, NB:, :].astype(jnp.float32)[0, 0].astype(jnp.int32) for s in at]
        for i, mark in enumerate(marks):
            total = even if i % 2 == 0 else odd
            total[mark] += slots[at[i], :NB, :].astype(jnp.float32)

    for i in range(ATOM_ROWS):
        for j in range(ATOM_COLS):
            keep = pattern_ref[i * ATOM_COLS + j] > 0
            block = even[i * ATOM_COLS + j + 1] + odd[i * ATOM_COLS + j + 1]
            full[i * NB : i * NB + NB, j * NB : j * NB + NB] = jnp.where(keep, block, 0.0).astype(
                jnp.bfloat16
            )


def hamiltonian_tile(pattern_tile, core, received):
    hbm = pl.BlockSpec(memory_space=pl.ANY)
    return pl.pallas_call(
        sum_kernel,
        in_specs=[SMEM, hbm, hbm],
        out_specs=pl.BlockSpec(memory_space=pltpu.VMEM),
        scratch_shapes=[
            pltpu.VMEM(core.shape, jnp.bfloat16),
            pltpu.VMEM(received.shape, jnp.bfloat16),
            pltpu.VMEM((ATOM_ROWS * ATOM_COLS + 1, NB, NB), jnp.float32),
            pltpu.VMEM((ATOM_ROWS * ATOM_COLS + 1, NB, NB), jnp.float32),
            pltpu.SemaphoreType.DMA,
            pltpu.SemaphoreType.DMA((SUM_GROUPS,)),
        ],
        out_shape=jax.ShapeDtypeStruct(core.shape, jnp.bfloat16),
        name="sum_blocks",
    )(pattern_tile, core, received)


def product_kernel(count, first, has_acc, index, *refs):
    pieces, stacks = refs[:count], refs[count : count + 4]
    acc = refs[count + 4] if has_acc else None
    out, columns, rows, total, column_sem, row_sem, acc_sem, out_sem = refs[-8:]
    mine = pl.multiple_of(index[0] * 512, 512)
    theirs = pl.multiple_of(512 - index[0] * 512, 512)

    for k in range(count):
        pltpu.make_async_copy(pieces[k], columns.at[k], column_sem.at[k]).start()
        for s, (base, at) in enumerate(((1, mine), (9, theirs))):
            tile = index[base + first + k]
            for half in range(2):

                @pl.when(tile >> 2 == half)
                def _(k=k, s=s, at=at, tile=tile, half=half):
                    pltpu.make_async_copy(
                        stacks[2 * s + half].at[tile & 3],
                        rows.at[k, pl.ds(at, 512), :],
                        row_sem.at[k, s],
                    ).start()

    if has_acc:
        load = pltpu.make_async_copy(acc, total, acc_sem)
        load.start()
    else:
        total[...] = jnp.zeros_like(total)

    def arrive(k):
        pltpu.make_async_copy(pieces[0], columns.at[k], column_sem.at[k]).wait()
        for s, at in enumerate((mine, theirs)):
            pltpu.make_async_copy(
                stacks[0].at[0], rows.at[k, pl.ds(at, 512), :], row_sem.at[k, s]
            ).wait()

    if has_acc:
        load.wait()

    @pl.loop(0, count - 1)
    def _(k):
        arrive(k)
        total[...] += jnp.dot(columns[k], rows[k], preferred_element_type=jnp.float32)

    last = count - 1
    arrive(last)
    writes = []
    for p in range(2):
        part = slice(256 * p, 256 * p + 256)
        total[part, :] += jnp.dot(
            columns[last, part, :], rows[last], preferred_element_type=jnp.float32
        )
        writes.append(
            pltpu.make_async_copy(total.at[part, :], out.at[part, :], out_sem.at[p])
        )
        writes[-1].start()
    for write in writes:
        write.wait()


def multiply(index, first, acc, pieces, stacks):
    count = len(pieces)
    given = [] if acc is None else [acc]
    hbm = pl.BlockSpec(memory_space=pl.ANY)
    return pl.pallas_call(
        functools.partial(product_kernel, count, first, acc is not None),
        in_specs=[SMEM] + [hbm] * (count + 4 + len(given)),
        out_specs=hbm,
        scratch_shapes=[
            pltpu.VMEM((count, 512, 1024), jnp.bfloat16),
            pltpu.VMEM((count, 1024, 1024), jnp.bfloat16),
            pltpu.VMEM((512, 1024), jnp.float32),
            pltpu.SemaphoreType.DMA((count,)),
            pltpu.SemaphoreType.DMA((count, 2)),
            pltpu.SemaphoreType.DMA,
            pltpu.SemaphoreType.DMA((2,)),
        ],
        out_shape=jax.ShapeDtypeStruct((512, 1024), jnp.float32),
        name="product",
    )(index, *pieces, *stacks, *given)


def block_mask(values, pattern_tile, block_size):
    row_blocks, col_blocks = pattern_tile.shape
    shaped = values.reshape(row_blocks, block_size, col_blocks, block_size)
    selected = (pattern_tile > 0)[:, None, :, None]
    kept = jnp.where(selected, shaped, jnp.zeros((), values.dtype))
    return kept.reshape(row_blocks * block_size, col_blocks * block_size)


Z_ROUTES = (
    (0, (0, 1), (0, 1)),
    (0, (1, 0), (-1, 0)),
    (0, (-1, 0), (1, 0)),
    (1, (-1, 0), (1, 0)),
    (1, (1, 0), (-1, 0)),
    (2, (1, 0), (-1, 0)),
    (4, (-1, 0), (1, 0)),
)
X_ROUTES = (
    (0, (0, 1), (1, 0)),
    (0, (1, 0), (-1, 0)),
    (0, (-1, 0), (0, 1)),
    (1, (-1, 0), (1, 0)),
    (1, (1, 0), (0, 1)),
    (2, (1, 0), (0, 1)),
    (4, (-1, 0), (0, 1)),
)


def come_from(routes, core):
    found = [(0, 0)]
    for source, *moves in routes:
        steps, cross = moves[core]
        at = found[source]
        found.append(((at[0] - steps) % 4, (at[1] + cross) % 2))
    return found


def tile_at(routes, core):
    found = come_from(routes, core)
    return [found.index((i % 4, i // 4)) for i in range(8)]


def send(array, ring, k):
    _, *moves = (Z_ROUTES if ring == "z" else X_ROUTES)[k]
    axes = ("yl", "z", "c") if ring == "z" else ("c", "x", "yh")
    pairs = []
    for c in range(2):
        steps, cross = moves[c]
        for i in range(4):
            for y in range(2):
                to_i, to_y = (i + steps) % 4, (y + cross) % 2
                if ring == "z":
                    pairs.append(((y * 4 + i) * 2 + c, (to_y * 4 + to_i) * 2 + c))
                else:
                    pairs.append(((c * 4 + i) * 2 + y, (c * 4 + to_i) * 2 + to_y))
    return lax.ppermute(array, axes, pairs)


def steps(
    potential, basis_left, basis_right, core_matrix, density, pattern, pair_atoms, cube_offsets,
    live_count,
):
    x, yh = lax.axis_index("x"), lax.axis_index("yh")
    yl, z, c = lax.axis_index("yl"), lax.axis_index("z"), lax.axis_index("c")

    offsets = cube_offsets.T
    prev_offsets = shift(offsets, ALL, 1)
    next_offsets = shift(offsets, ALL, -1)

    d = [density]
    for k in range(7):
        d.append(send(d[Z_ROUTES[k][0]], "z", k))

    for_prev, for_next = cut_edges(prev_offsets, next_offsets, potential)
    high = shift(for_prev, ALL, -1)
    low = shift(for_next, ALL, 1)
    own = cut_own(offsets, potential)
    outgoing = partial_blocks(
        pair_atoms.T, live_count, offsets, low, own, high, basis_left, basis_right
    )
    received = lax.all_to_all(outgoing, ALL, 0, 0, tiled=True)

    column = lax.axis_index(COL) * ATOM_COLS
    origins = jnp.where(
        c == 0, jnp.array(come_from(Z_ROUTES, 0)), jnp.array(come_from(Z_ROUTES, 1))
    )
    origin_rows = ((((yl + origins[:, 1]) & 1) * 4 + ((z + origins[:, 0]) & 3)) * 2 + c) * ATOM_ROWS

    def masked(tiles, first):
        return jnp.stack(
            [
                block_mask(
                    tile,
                    lax.dynamic_slice(
                        pattern, (origin_rows[first + k], column), (ATOM_ROWS, ATOM_COLS)
                    ),
                    NB,
                )
                for k, tile in enumerate(tiles)
            ]
        )

    early = masked(d[:4], 0)
    early_other = shift(early, "c", 1)

    corner = (lax.axis_index(ROW) * ATOM_ROWS, column)
    pattern_tile = lax.dynamic_slice(pattern, corner, (ATOM_ROWS, ATOM_COLS))
    hamiltonian = hamiltonian_tile(pattern_tile.reshape(-1), core_matrix, received)
    h = [hamiltonian]
    for k in range(7):
        h.append(send(h[X_ROUTES[k][0]], "x", k))

    late_tiles = lax.optimization_barrier((*d[4:], hamiltonian))[:4]
    late = masked(late_tiles, 4)
    late_other = shift(late, "c", 1)
    stacks = (early, late, early_other, late_other)

    sources = jnp.where(c == 0, jnp.array(come_from(X_ROUTES, 0)), jnp.array(come_from(X_ROUTES, 1)))
    block = ((x + sources[:, 0]) & 3) * 2 + ((yh + sources[:, 1]) & 1)
    at = (((block >> 2) + yl) & 1) * 4 + ((block - z) & 3)
    first, second = jnp.array(tile_at(Z_ROUTES, 0)), jnp.array(tile_at(Z_ROUTES, 1))
    hot = (at[:, None] == jnp.arange(8)[None, :]).astype(jnp.int32)
    in_own = jnp.sum(hot * jnp.where(c == 0, first, second)[None, :], axis=1)
    in_other = jnp.sum(hot * jnp.where(c == 0, second, first)[None, :], axis=1)
    index = jnp.concatenate([c.reshape(1), in_own, in_other]).astype(jnp.int32)

    out = multiply(index, 0, None, h[:4], stacks)
    out = multiply(index, 4, out, h[4:7], stacks)
    out = multiply(index, 7, out, h[7:], stacks)
    return hamiltonian, out


def solution(mesh):
    split = Mesh(mesh.devices.reshape(2, 4, 2, 4, 2), ALL)
    placed = (
        P(ALL, None, None),
        P(ALL, None, None),
        P(ALL, None, None),
        P(ROW, COL),
        P(ROW, COL),
        P(),
        P(ALL, None),
        P(ALL, None),
        P(ALL),
    )
    return jax.shard_map(
        steps,
        mesh=split,
        in_specs=placed,
        out_specs=(P(ROW, COL), P(ROW, COL)),
        check_vma=False,
    )
```

```python
import functools

import jax
import jax.numpy as jnp
from jax import lax
from jax.experimental import pallas as pl
from jax.experimental.pallas import tpu as pltpu
from jax.sharding import Mesh
from jax.sharding import PartitionSpec as P


NB = 128
ENTRIES = 64
DEVICES = 128
ATOM_ROWS = 4
ATOM_COLS = 8
CELLS = 384
ROW = ("yl", "z", "c")
COL = ("x", "yh")
ALL = ("yl", "z", "c", "x", "yh")


SMEM = pl.BlockSpec(memory_space=pltpu.SMEM)


def shift(array, axis, step):
    size = lax.axis_size(axis)
    return lax.ppermute(array, axis, [(i, (i + step) % size) for i in range(size)])


def turned_pair(slab, first_plane, y0, z0):
    tile = z0 >> 7
    within = z0 & 127
    tile_after = jnp.minimum(tile + 1, 3)
    lane = lax.broadcasted_iota(jnp.int32, (8, 128), 1)
    planes = []
    for k in range(2):
        plane = 2048 * (first_plane + k) + y0
        here = slab[pl.ds(plane + 512 * tile, 8), :]
        after = slab[pl.ds(plane + 512 * tile_after, 8), :]
        turn = (128 + 64 * k - within) & 127
        planes.append(pltpu.roll(jnp.where(lane >= within, here, after), turn, 1))
    return jnp.where(lane < 64, planes[0], planes[1])


def as_rows(windows):
    lane = lax.broadcasted_iota(jnp.int32, windows.shape, 1)
    sub = lax.broadcasted_iota(jnp.int32, windows.shape, 0) & 7
    for bit in range(3):
        windows = jnp.where((sub >> bit) & 1 == 1, pltpu.roll(windows, 8 << bit, 1), windows)
    windows = jnp.where((lane >> 3) & 7 == sub, windows, 0.0)
    return jnp.sum(windows.reshape(-1, 8, 128), axis=1)


def column_copies(potential, slab, sem):
    return [
        pltpu.make_async_copy(
            potential.at[p, :, 128 * t : 128 * t + 128],
            slab.at[(p * 4 + t) * 512 : (p * 4 + t) * 512 + 512, :],
            sem.at[p * 4 + t],
        )
        for p in range(4)
        for t in range(4)
    ]


def cut_both(offset_refs, outs, potential, slab, held, sem):
    copies = column_copies(potential, slab, sem)
    for copy in copies:
        copy.start()
    for k in range(2):
        for copy in copies[8 * k : 8 * k + 8]:
            copy.wait()
        offset_ref = offset_refs[k]

        @pl.loop(0, ENTRIES, unroll=8)
        def _(e, k=k, offset_ref=offset_ref):
            row = pl.multiple_of(e * 8, 8)
            held[k, pl.ds(row, 8), :] = turned_pair(
                slab, 2 * k, offset_ref[1, e], offset_ref[2, e]
            )

        outs[k][...] = as_rows(held[k])


def edge_kernel(prev_ref, next_ref, potential, prev_out, next_out, slab, held, sem):
    cut_both((prev_ref, next_ref), (prev_out, next_out), potential, slab, held, sem)


def own_kernel(own_ref, potential, out, slab, held, sem):
    cut_both((own_ref, own_ref), (out.at[0], out.at[1]), potential, slab, held, sem)


CUT_SCRATCH = [
    pltpu.VMEM((16 * 512, 128), jnp.float32),
    pltpu.VMEM((2, ENTRIES * 8, 128), jnp.float32),
    pltpu.SemaphoreType.DMA((16,)),
]


def cut_edges(prev_offsets, next_offsets, potential):
    shape = jax.ShapeDtypeStruct((ENTRIES, 128), jnp.float32)
    return pl.pallas_call(
        edge_kernel,
        out_shape=(shape, shape),
        in_specs=[SMEM, SMEM, pl.BlockSpec(memory_space=pl.ANY)],
        scratch_shapes=CUT_SCRATCH,
        name="cut_edges",
    )(prev_offsets, next_offsets, potential)


def cut_own(offsets, potential):
    return pl.pallas_call(
        own_kernel,
        out_shape=jax.ShapeDtypeStruct((2, ENTRIES, 128), jnp.float32),
        in_specs=[SMEM, pl.BlockSpec(memory_space=pl.ANY)],
        scratch_shapes=CUT_SCRATCH,
        name="cut_own",
    )(offsets, potential)


GROUP = 8
GROUPS = ENTRIES // GROUP
TAIL = 8


def cube_row(windows, along):
    lane = lax.broadcasted_iota(jnp.int32, (1, 128), 1)
    turned = [pltpu.roll(w, 64, 1) for w in windows]
    cells = []
    for i in range(3):
        between = jnp.where(lane < 64, turned[i], turned[i + 1])
        cells.append(
            jnp.where(along == 0, windows[i], jnp.where(along == 1, between, windows[i + 1]))
        )
    return jnp.concatenate(cells, axis=1)


def partial_kernel(
    pair_ref, live_ref, offset_ref, low, own, high, left, right, out,
    lefts, rights, staged, blank, in_sem, out_sem, blank_sem,
):
    def reads(g):
        rows = pl.ds(g * GROUP, GROUP)
        return (
            pltpu.make_async_copy(left.at[rows], lefts.at[rows], in_sem.at[g, 0]),
            pltpu.make_async_copy(right.at[rows], rights.at[rows], in_sem.at[g, 1]),
        )

    for g in range(GROUPS):
        for copy in reads(g):
            copy.start()
    blank[...] = jnp.zeros_like(blank)
    clear = pltpu.make_async_copy(blank, out.at[:, NB:, :], blank_sem)
    clear.start()
    clear.wait()

    @pl.loop(0, GROUPS)
    def _(g):
        for copy in reads(g):
            copy.wait()
        for i in range(GROUP):
            e = g * GROUP + i
            row = pl.ds(e, 1)
            windows = [low[row, :], own[0, row, :], own[1, row, :], high[row, :]]
            cube = cube_row(windows, offset_ref[0, e])
            weighted = (lefts[e].astype(jnp.float32) * cube).astype(jnp.bfloat16)
            block = lax.dot_general(
                weighted, rights[e], (((1,), (1,)), ((), ())), preferred_element_type=jnp.float32
            )
            first, second = pair_ref[0, e], pair_ref[1, e]
            owner = (first >> 2) * 8 + (second >> 3)
            mark = jnp.where(e < live_ref[0], (first & 3) * ATOM_COLS + (second & 7) + 1, 0)
            staged[e, :NB, :] = block.astype(jnp.bfloat16)
            staged[e, NB:, :] = jnp.full((TAIL, NB), mark.astype(jnp.float32)).astype(jnp.bfloat16)
            pltpu.make_async_copy(staged.at[e], out.at[owner], out_sem.at[e]).start()

    @pl.loop(0, ENTRIES)
    def _(e):
        pltpu.make_async_copy(staged.at[e], out.at[0], out_sem.at[e]).wait()


def partial_blocks(pairs, live, offsets, low, own, high, left, right):
    vmem = pl.BlockSpec(memory_space=pltpu.VMEM)
    hbm = pl.BlockSpec(memory_space=pl.ANY)
    return pl.pallas_call(
        partial_kernel,
        in_specs=[SMEM] * 3 + [vmem] * 3 + [hbm] * 2,
        out_specs=hbm,
        scratch_shapes=[
            pltpu.VMEM((ENTRIES, NB, CELLS), jnp.bfloat16),
            pltpu.VMEM((ENTRIES, NB, CELLS), jnp.bfloat16),
            pltpu.VMEM((ENTRIES, NB + TAIL, NB), jnp.bfloat16),
            pltpu.VMEM((DEVICES, TAIL, NB), jnp.bfloat16),
            pltpu.SemaphoreType.DMA((GROUPS, 2)),
            pltpu.SemaphoreType.DMA((ENTRIES,)),
            pltpu.SemaphoreType.DMA,
        ],
        out_shape=jax.ShapeDtypeStruct((DEVICES, NB + TAIL, NB), jnp.bfloat16),
        name="partial_blocks",
    )(pairs, live, offsets, low, own, high, left, right)


SUM_GROUP = 16
SUM_GROUPS = DEVICES // SUM_GROUP


def sum_kernel(pattern_ref, core, received, full, tile, slots, even, odd, core_sem, slot_sem):
    def read(g):
        rows = pl.ds(g * SUM_GROUP, SUM_GROUP)
        return pltpu.make_async_copy(received.at[rows], slots.at[rows], slot_sem.at[g])

    load = pltpu.make_async_copy(core, tile, core_sem)
    load.start()
    for g in range(SUM_GROUPS):
        read(g).start()
    odd[...] = jnp.zeros_like(odd)
    load.wait()
    for i in range(ATOM_ROWS):
        for j in range(ATOM_COLS):
            block = tile[i * NB : i * NB + NB, j * NB : j * NB + NB]
            even[i * ATOM_COLS + j + 1] = block.astype(jnp.float32)

    @pl.loop(0, SUM_GROUPS)
    def _(g):
        read(g).wait()
        at = [g * SUM_GROUP + i for i in range(SUM_GROUP)]
        marks = [slots[s, NB:, :].astype(jnp.float32)[0, 0].astype(jnp.int32) for s in at]
        for i, mark in enumerate(marks):
            total = even if i % 2 == 0 else odd
            total[mark] += slots[at[i], :NB, :].astype(jnp.float32)

    for i in range(ATOM_ROWS):
        for j in range(ATOM_COLS):
            keep = pattern_ref[i * ATOM_COLS + j] > 0
            block = even[i * ATOM_COLS + j + 1] + odd[i * ATOM_COLS + j + 1]
            full[i * NB : i * NB + NB, j * NB : j * NB + NB] = jnp.where(keep, block, 0.0).astype(
                jnp.bfloat16
            )


def hamiltonian_tile(pattern_tile, core, received):
    hbm = pl.BlockSpec(memory_space=pl.ANY)
    return pl.pallas_call(
        sum_kernel,
        in_specs=[SMEM, hbm, hbm],
        out_specs=pl.BlockSpec(memory_space=pltpu.VMEM),
        scratch_shapes=[
            pltpu.VMEM(core.shape, jnp.bfloat16),
            pltpu.VMEM(received.shape, jnp.bfloat16),
            pltpu.VMEM((ATOM_ROWS * ATOM_COLS + 1, NB, NB), jnp.float32),
            pltpu.VMEM((ATOM_ROWS * ATOM_COLS + 1, NB, NB), jnp.float32),
            pltpu.SemaphoreType.DMA,
            pltpu.SemaphoreType.DMA((SUM_GROUPS,)),
        ],
        out_shape=jax.ShapeDtypeStruct(core.shape, jnp.bfloat16),
        name="sum_blocks",
    )(pattern_tile, core, received)


def product_kernel(count, first, has_acc, index, *refs):
    pieces, stacks = refs[:count], refs[count : count + 4]
    acc = refs[count + 4] if has_acc else None
    out, columns, rows, total, column_sem, row_sem, acc_sem, out_sem = refs[-8:]
    mine = pl.multiple_of(index[0] * 512, 512)
    theirs = pl.multiple_of(512 - index[0] * 512, 512)

    for k in range(count):
        pltpu.make_async_copy(pieces[k], columns.at[k], column_sem.at[k]).start()
        for s, (base, at) in enumerate(((1, mine), (9, theirs))):
            tile = index[base + first + k]
            for half in range(2):

                @pl.when(tile >> 2 == half)
                def _(k=k, s=s, at=at, tile=tile, half=half):
                    pltpu.make_async_copy(
                        stacks[2 * s + half].at[tile & 3],
                        rows.at[k, pl.ds(at, 512), :],
                        row_sem.at[k, s],
                    ).start()

    if has_acc:
        load = pltpu.make_async_copy(acc, total, acc_sem)
        load.start()
    else:
        total[...] = jnp.zeros_like(total)

    def arrive(k):
        pltpu.make_async_copy(pieces[0], columns.at[k], column_sem.at[k]).wait()
        for s, at in enumerate((mine, theirs)):
            pltpu.make_async_copy(
                stacks[0].at[0], rows.at[k, pl.ds(at, 512), :], row_sem.at[k, s]
            ).wait()

    if has_acc:
        load.wait()

    @pl.loop(0, count - 1)
    def _(k):
        arrive(k)
        total[...] += jnp.dot(columns[k], rows[k], preferred_element_type=jnp.float32)

    last = count - 1
    arrive(last)
    writes = []
    for p in range(2):
        part = slice(256 * p, 256 * p + 256)
        total[part, :] += jnp.dot(
            columns[last, part, :], rows[last], preferred_element_type=jnp.float32
        )
        writes.append(
            pltpu.make_async_copy(total.at[part, :], out.at[part, :], out_sem.at[p])
        )
        writes[-1].start()
    for write in writes:
        write.wait()


def multiply(index, first, acc, pieces, stacks):
    count = len(pieces)
    given = [] if acc is None else [acc]
    hbm = pl.BlockSpec(memory_space=pl.ANY)
    return pl.pallas_call(
        functools.partial(product_kernel, count, first, acc is not None),
        in_specs=[SMEM]
        + [pl.BlockSpec(memory_space=pltpu.HBM)] * (count + 4)
        + [hbm] * len(given),
        out_specs=hbm,
        scratch_shapes=[
            pltpu.VMEM((count, 512, 1024), jnp.bfloat16),
            pltpu.VMEM((count, 1024, 1024), jnp.bfloat16),
            pltpu.VMEM((512, 1024), jnp.float32),
            pltpu.SemaphoreType.DMA((count,)),
            pltpu.SemaphoreType.DMA((count, 2)),
            pltpu.SemaphoreType.DMA,
            pltpu.SemaphoreType.DMA((2,)),
        ],
        out_shape=jax.ShapeDtypeStruct((512, 1024), jnp.float32),
        name="product",
    )(index, *pieces, *stacks, *given)


def block_mask(values, pattern_tile, block_size):
    row_blocks, col_blocks = pattern_tile.shape
    shaped = values.reshape(row_blocks, block_size, col_blocks, block_size)
    selected = (pattern_tile > 0)[:, None, :, None]
    kept = jnp.where(selected, shaped, jnp.zeros((), values.dtype))
    return kept.reshape(row_blocks * block_size, col_blocks * block_size)


Z_ROUTES = (
    (0, (0, 1), (0, 1)),
    (0, (1, 0), (-1, 0)),
    (0, (-1, 0), (1, 0)),
    (1, (-1, 0), (1, 0)),
    (1, (1, 0), (-1, 0)),
    (2, (1, 0), (-1, 0)),
    (4, (-1, 0), (1, 0)),
)
X_ROUTES = (
    (0, (0, 1), (1, 0)),
    (0, (-1, 0), (-1, 0)),
    (0, (1, 0), (0, 1)),
    (1, (-1, 0), (1, 0)),
    (1, (1, 0), (0, 1)),
    (2, (-1, 0), (0, 1)),
    (4, (-1, 0), (0, 1)),
)


def come_from(routes, core):
    found = [(0, 0)]
    for source, *moves in routes:
        steps, cross = moves[core]
        at = found[source]
        found.append(((at[0] - steps) % 4, (at[1] + cross) % 2))
    return found


def tile_at(routes, core):
    found = come_from(routes, core)
    return [found.index((i % 4, i // 4)) for i in range(8)]


def send(array, ring, k):
    _, *moves = (Z_ROUTES if ring == "z" else X_ROUTES)[k]
    axes = ("yl", "z", "c") if ring == "z" else ("c", "x", "yh")
    pairs = []
    for c in range(2):
        steps, cross = moves[c]
        for i in range(4):
            for y in range(2):
                to_i, to_y = (i + steps) % 4, (y + cross) % 2
                if ring == "z":
                    pairs.append(((y * 4 + i) * 2 + c, (to_y * 4 + to_i) * 2 + c))
                else:
                    pairs.append(((c * 4 + i) * 2 + y, (c * 4 + to_i) * 2 + to_y))
    return lax.ppermute(array, axes, pairs)


def steps(
    potential, basis_left, basis_right, core_matrix, density, pattern, pair_atoms, cube_offsets,
    live_count,
):
    x, yh = lax.axis_index("x"), lax.axis_index("yh")
    yl, z, c = lax.axis_index("yl"), lax.axis_index("z"), lax.axis_index("c")

    offsets = cube_offsets.T
    prev_offsets = shift(offsets, ALL, 1)
    next_offsets = shift(offsets, ALL, -1)

    d = [density]
    for k in range(7):
        d.append(send(d[Z_ROUTES[k][0]], "z", k))

    for_prev, for_next = cut_edges(prev_offsets, next_offsets, potential)
    high = shift(for_prev, ALL, -1)
    low = shift(for_next, ALL, 1)
    own = cut_own(offsets, potential)
    outgoing = partial_blocks(
        pair_atoms.T, live_count, offsets, low, own, high, basis_left, basis_right
    )
    received = lax.all_to_all(outgoing, ALL, 0, 0, tiled=True)

    column = lax.axis_index(COL) * ATOM_COLS
    origins = jnp.where(
        c == 0, jnp.array(come_from(Z_ROUTES, 0)), jnp.array(come_from(Z_ROUTES, 1))
    )
    origin_rows = ((((yl + origins[:, 1]) & 1) * 4 + ((z + origins[:, 0]) & 3)) * 2 + c) * ATOM_ROWS

    def masked(tiles, first):
        return jnp.stack(
            [
                block_mask(
                    tile,
                    lax.dynamic_slice(
                        pattern, (origin_rows[first + k], column), (ATOM_ROWS, ATOM_COLS)
                    ),
                    NB,
                )
                for k, tile in enumerate(tiles)
            ]
        )

    early = masked(d[:4], 0)
    early_other = shift(early, "c", 1)

    corner = (lax.axis_index(ROW) * ATOM_ROWS, column)
    pattern_tile = lax.dynamic_slice(pattern, corner, (ATOM_ROWS, ATOM_COLS))
    hamiltonian = hamiltonian_tile(pattern_tile.reshape(-1), core_matrix, received)
    h = [hamiltonian]
    for k in range(7):
        h.append(send(h[X_ROUTES[k][0]], "x", k))

    late_tiles = lax.optimization_barrier((*d[4:], hamiltonian))[:4]
    late = masked(late_tiles, 4)
    late_other = shift(late, "c", 1)
    stacks = (early, late, early_other, late_other)

    sources = jnp.where(c == 0, jnp.array(come_from(X_ROUTES, 0)), jnp.array(come_from(X_ROUTES, 1)))
    block = ((x + sources[:, 0]) & 3) * 2 + ((yh + sources[:, 1]) & 1)
    at = (((block >> 2) + yl) & 1) * 4 + ((block - z) & 3)
    first, second = jnp.array(tile_at(Z_ROUTES, 0)), jnp.array(tile_at(Z_ROUTES, 1))
    hot = (at[:, None] == jnp.arange(8)[None, :]).astype(jnp.int32)
    in_own = jnp.sum(hot * jnp.where(c == 0, first, second)[None, :], axis=1)
    in_other = jnp.sum(hot * jnp.where(c == 0, second, first)[None, :], axis=1)
    index = jnp.concatenate([c.reshape(1), in_own, in_other]).astype(jnp.int32)

    out = multiply(index, 0, None, h[:4], stacks)
    out = multiply(index, 4, out, h[4:7], stacks)
    out = multiply(index, 7, out, h[7:], stacks)
    return hamiltonian, out


def solution(mesh):
    split = Mesh(mesh.devices.reshape(2, 4, 2, 4, 2), ALL)
    placed = (
        P(ALL, None, None),
        P(ALL, None, None),
        P(ALL, None, None),
        P(ROW, COL),
        P(ROW, COL),
        P(),
        P(ALL, None),
        P(ALL, None),
        P(ALL),
    )
    return jax.shard_map(
        steps,
        mesh=split,
        in_specs=placed,
        out_specs=(P(ROW, COL), P(ROW, COL)),
        check_vma=False,
    )
```

```python
import functools

import jax
import jax.numpy as jnp
from jax import lax
from jax.experimental import pallas as pl
from jax.experimental.pallas import tpu as pltpu
from jax.sharding import Mesh
from jax.sharding import PartitionSpec as P


NB = 128
ENTRIES = 64
DEVICES = 128
ATOM_ROWS = 4
ATOM_COLS = 8
CELLS = 384
ROW = ("yl", "z", "c")
COL = ("x", "yh")
ALL = ("yl", "z", "c", "x", "yh")


SMEM = pl.BlockSpec(memory_space=pltpu.SMEM)


def shift(array, axis, step):
    size = lax.axis_size(axis)
    return lax.ppermute(array, axis, [(i, (i + step) % size) for i in range(size)])


def turned_pair(slab, first_plane, y0, z0):
    tile = z0 >> 7
    within = z0 & 127
    tile_after = jnp.minimum(tile + 1, 3)
    lane = lax.broadcasted_iota(jnp.int32, (8, 128), 1)
    planes = []
    for k in range(2):
        plane = 2048 * (first_plane + k) + y0
        here = slab[pl.ds(plane + 512 * tile, 8), :]
        after = slab[pl.ds(plane + 512 * tile_after, 8), :]
        turn = (128 + 64 * k - within) & 127
        planes.append(pltpu.roll(jnp.where(lane >= within, here, after), turn, 1))
    return jnp.where(lane < 64, planes[0], planes[1])


def as_rows(windows):
    lane = lax.broadcasted_iota(jnp.int32, windows.shape, 1)
    sub = lax.broadcasted_iota(jnp.int32, windows.shape, 0) & 7
    for bit in range(3):
        windows = jnp.where((sub >> bit) & 1 == 1, pltpu.roll(windows, 8 << bit, 1), windows)
    windows = jnp.where((lane >> 3) & 7 == sub, windows, 0.0)
    return jnp.sum(windows.reshape(-1, 8, 128), axis=1)


def column_copies(potential, slab, sem):
    return [
        pltpu.make_async_copy(
            potential.at[p, :, 128 * t : 128 * t + 128],
            slab.at[(p * 4 + t) * 512 : (p * 4 + t) * 512 + 512, :],
            sem.at[p * 4 + t],
        )
        for p in range(4)
        for t in range(4)
    ]


def cut_both(offset_refs, outs, potential, slab, held, sem):
    copies = column_copies(potential, slab, sem)
    for copy in copies:
        copy.start()
    for k in range(2):
        for copy in copies[8 * k : 8 * k + 8]:
            copy.wait()
        offset_ref = offset_refs[k]

        @pl.loop(0, ENTRIES, unroll=8)
        def _(e, k=k, offset_ref=offset_ref):
            row = pl.multiple_of(e * 8, 8)
            held[k, pl.ds(row, 8), :] = turned_pair(
                slab, 2 * k, offset_ref[1, e], offset_ref[2, e]
            )

        outs[k][...] = as_rows(held[k])


def edge_kernel(prev_ref, next_ref, potential, prev_out, next_out, slab, held, sem):
    cut_both((prev_ref, next_ref), (prev_out, next_out), potential, slab, held, sem)


def own_kernel(own_ref, potential, out, slab, held, sem):
    cut_both((own_ref, own_ref), (out.at[0], out.at[1]), potential, slab, held, sem)


CUT_SCRATCH = [
    pltpu.VMEM((16 * 512, 128), jnp.float32),
    pltpu.VMEM((2, ENTRIES * 8, 128), jnp.float32),
    pltpu.SemaphoreType.DMA((16,)),
]


def cut_edges(prev_offsets, next_offsets, potential):
    shape = jax.ShapeDtypeStruct((ENTRIES, 128), jnp.float32)
    return pl.pallas_call(
        edge_kernel,
        out_shape=(shape, shape),
        in_specs=[SMEM, SMEM, pl.BlockSpec(memory_space=pl.ANY)],
        scratch_shapes=CUT_SCRATCH,
        name="cut_edges",
    )(prev_offsets, next_offsets, potential)


def cut_own(offsets, potential):
    return pl.pallas_call(
        own_kernel,
        out_shape=jax.ShapeDtypeStruct((2, ENTRIES, 128), jnp.float32),
        in_specs=[SMEM, pl.BlockSpec(memory_space=pl.ANY)],
        scratch_shapes=CUT_SCRATCH,
        name="cut_own",
    )(offsets, potential)


GROUP = 8
GROUPS = ENTRIES // GROUP
TAIL = 8


def cube_row(windows, along):
    lane = lax.broadcasted_iota(jnp.int32, (1, 128), 1)
    turned = [pltpu.roll(w, 64, 1) for w in windows]
    cells = []
    for i in range(3):
        between = jnp.where(lane < 64, turned[i], turned[i + 1])
        cells.append(
            jnp.where(along == 0, windows[i], jnp.where(along == 1, between, windows[i + 1]))
        )
    return jnp.concatenate(cells, axis=1)


def partial_kernel(
    pair_ref, live_ref, offset_ref, low, own, high, left, right, out,
    lefts, rights, staged, blank, in_sem, out_sem, blank_sem,
):
    def reads(g):
        rows = pl.ds(g * GROUP, GROUP)
        return (
            pltpu.make_async_copy(left.at[rows], lefts.at[rows], in_sem.at[g, 0]),
            pltpu.make_async_copy(right.at[rows], rights.at[rows], in_sem.at[g, 1]),
        )

    for g in range(GROUPS):
        for copy in reads(g):
            copy.start()
    blank[...] = jnp.zeros_like(blank)
    clear = pltpu.make_async_copy(blank, out.at[:, NB:, :], blank_sem)
    clear.start()
    clear.wait()

    @pl.loop(0, GROUPS)
    def _(g):
        for copy in reads(g):
            copy.wait()
        for i in range(GROUP):
            e = g * GROUP + i
            row = pl.ds(e, 1)
            windows = [low[row, :], own[0, row, :], own[1, row, :], high[row, :]]
            cube = cube_row(windows, offset_ref[0, e])
            weighted = (lefts[e].astype(jnp.float32) * cube).astype(jnp.bfloat16)
            block = lax.dot_general(
                weighted, rights[e], (((1,), (1,)), ((), ())), preferred_element_type=jnp.float32
            )
            first, second = pair_ref[0, e], pair_ref[1, e]
            owner = (first >> 2) * 8 + (second >> 3)
            mark = jnp.where(e < live_ref[0], (first & 3) * ATOM_COLS + (second & 7) + 1, 0)
            staged[e, :NB, :] = block.astype(jnp.bfloat16)
            staged[e, NB:, :] = jnp.full((TAIL, NB), mark.astype(jnp.float32)).astype(jnp.bfloat16)
            pltpu.make_async_copy(staged.at[e], out.at[owner], out_sem.at[e]).start()

    @pl.loop(0, ENTRIES)
    def _(e):
        pltpu.make_async_copy(staged.at[e], out.at[0], out_sem.at[e]).wait()


def partial_blocks(pairs, live, offsets, low, own, high, left, right):
    vmem = pl.BlockSpec(memory_space=pltpu.VMEM)
    hbm = pl.BlockSpec(memory_space=pl.ANY)
    return pl.pallas_call(
        partial_kernel,
        in_specs=[SMEM] * 3 + [vmem] * 3 + [hbm] * 2,
        out_specs=hbm,
        scratch_shapes=[
            pltpu.VMEM((ENTRIES, NB, CELLS), jnp.bfloat16),
            pltpu.VMEM((ENTRIES, NB, CELLS), jnp.bfloat16),
            pltpu.VMEM((ENTRIES, NB + TAIL, NB), jnp.bfloat16),
            pltpu.VMEM((DEVICES, TAIL, NB), jnp.bfloat16),
            pltpu.SemaphoreType.DMA((GROUPS, 2)),
            pltpu.SemaphoreType.DMA((ENTRIES,)),
            pltpu.SemaphoreType.DMA,
        ],
        out_shape=jax.ShapeDtypeStruct((DEVICES, NB + TAIL, NB), jnp.bfloat16),
        name="partial_blocks",
    )(pairs, live, offsets, low, own, high, left, right)


SUM_GROUP = 16
SUM_GROUPS = DEVICES // SUM_GROUP


def sum_kernel(pattern_ref, core, received, full, tile, slots, even, odd, core_sem, slot_sem):
    def read(g):
        rows = pl.ds(g * SUM_GROUP, SUM_GROUP)
        return pltpu.make_async_copy(received.at[rows], slots.at[rows], slot_sem.at[g])

    load = pltpu.make_async_copy(core, tile, core_sem)
    load.start()
    for g in range(SUM_GROUPS):
        read(g).start()
    odd[...] = jnp.zeros_like(odd)
    load.wait()
    for i in range(ATOM_ROWS):
        for j in range(ATOM_COLS):
            block = tile[i * NB : i * NB + NB, j * NB : j * NB + NB]
            even[i * ATOM_COLS + j + 1] = block.astype(jnp.float32)

    @pl.loop(0, SUM_GROUPS)
    def _(g):
        read(g).wait()
        at = [g * SUM_GROUP + i for i in range(SUM_GROUP)]
        marks = [slots[s, NB:, :].astype(jnp.float32)[0, 0].astype(jnp.int32) for s in at]
        for i, mark in enumerate(marks):
            total = even if i % 2 == 0 else odd
            total[mark] += slots[at[i], :NB, :].astype(jnp.float32)

    for i in range(ATOM_ROWS):
        for j in range(ATOM_COLS):
            keep = pattern_ref[i * ATOM_COLS + j] > 0
            block = even[i * ATOM_COLS + j + 1] + odd[i * ATOM_COLS + j + 1]
            full[i * NB : i * NB + NB, j * NB : j * NB + NB] = jnp.where(keep, block, 0.0).astype(
                jnp.bfloat16
            )


def hamiltonian_tile(pattern_tile, core, received):
    hbm = pl.BlockSpec(memory_space=pl.ANY)
    return pl.pallas_call(
        sum_kernel,
        in_specs=[SMEM, hbm, hbm],
        out_specs=pl.BlockSpec(memory_space=pltpu.VMEM),
        scratch_shapes=[
            pltpu.VMEM(core.shape, jnp.bfloat16),
            pltpu.VMEM(received.shape, jnp.bfloat16),
            pltpu.VMEM((ATOM_ROWS * ATOM_COLS + 1, NB, NB), jnp.float32),
            pltpu.VMEM((ATOM_ROWS * ATOM_COLS + 1, NB, NB), jnp.float32),
            pltpu.SemaphoreType.DMA,
            pltpu.SemaphoreType.DMA((SUM_GROUPS,)),
        ],
        out_shape=jax.ShapeDtypeStruct(core.shape, jnp.bfloat16),
        name="sum_blocks",
    )(pattern_tile, core, received)


def product_kernel(count, first, has_acc, index, *refs):
    pieces, stacks = refs[:count], refs[count : count + 4]
    acc = refs[count + 4] if has_acc else None
    out, columns, rows, total, column_sem, row_sem, acc_sem, out_sem = refs[-8:]
    mine = pl.multiple_of(index[0] * 512, 512)
    theirs = pl.multiple_of(512 - index[0] * 512, 512)

    if has_acc:
        load = pltpu.make_async_copy(acc, total, acc_sem)
        load.start()
    else:
        total[...] = jnp.zeros_like(total)

    for k in range(count):
        pltpu.make_async_copy(pieces[k], columns.at[k], column_sem.at[k]).start()
        for s, (base, at) in enumerate(((1, mine), (9, theirs))):
            tile = index[base + first + k]
            for half in range(2):

                @pl.when(tile >> 2 == half)
                def _(k=k, s=s, at=at, tile=tile, half=half):
                    pltpu.make_async_copy(
                        stacks[2 * s + half].at[tile & 3],
                        rows.at[k, pl.ds(at, 512), :],
                        row_sem.at[k, s],
                    ).start()

    def arrive(k):
        pltpu.make_async_copy(pieces[0], columns.at[k], column_sem.at[k]).wait()
        for s, at in enumerate((mine, theirs)):
            pltpu.make_async_copy(
                stacks[0].at[0], rows.at[k, pl.ds(at, 512), :], row_sem.at[k, s]
            ).wait()

    if has_acc:
        load.wait()

    @pl.loop(0, count - 1)
    def _(k):
        arrive(k)
        total[...] += jnp.dot(columns[k], rows[k], preferred_element_type=jnp.float32)

    last = count - 1
    arrive(last)
    writes = []
    for p in range(2):
        part = slice(256 * p, 256 * p + 256)
        total[part, :] += jnp.dot(
            columns[last, part, :], rows[last], preferred_element_type=jnp.float32
        )
        writes.append(
            pltpu.make_async_copy(total.at[part, :], out.at[part, :], out_sem.at[p])
        )
        writes[-1].start()
    for write in writes:
        write.wait()


def multiply(index, first, acc, pieces, stacks):
    count = len(pieces)
    given = [] if acc is None else [acc]
    hbm = pl.BlockSpec(memory_space=pl.ANY)
    return pl.pallas_call(
        functools.partial(product_kernel, count, first, acc is not None),
        in_specs=[SMEM]
        + [pl.BlockSpec(memory_space=pltpu.HBM)] * (count + 4)
        + [hbm] * len(given),
        out_specs=hbm,
        scratch_shapes=[
            pltpu.VMEM((count, 512, 1024), jnp.bfloat16),
            pltpu.VMEM((count, 1024, 1024), jnp.bfloat16),
            pltpu.VMEM((512, 1024), jnp.float32),
            pltpu.SemaphoreType.DMA((count,)),
            pltpu.SemaphoreType.DMA((count, 2)),
            pltpu.SemaphoreType.DMA,
            pltpu.SemaphoreType.DMA((2,)),
        ],
        out_shape=jax.ShapeDtypeStruct((512, 1024), jnp.float32),
        name="product",
    )(index, *pieces, *stacks, *given)


def block_mask(values, pattern_tile, block_size):
    row_blocks, col_blocks = pattern_tile.shape
    shaped = values.reshape(row_blocks, block_size, col_blocks, block_size)
    selected = (pattern_tile > 0)[:, None, :, None]
    kept = jnp.where(selected, shaped, jnp.zeros((), values.dtype))
    return kept.reshape(row_blocks * block_size, col_blocks * block_size)


Z_ROUTES = (
    (0, (0, 1), (0, 1)),
    (0, (1, 0), (-1, 0)),
    (0, (-1, 0), (1, 0)),
    (1, (-1, 0), (1, 0)),
    (1, (1, 0), (-1, 0)),
    (2, (1, 0), (-1, 0)),
    (4, (-1, 0), (1, 0)),
)
X_ROUTES = (
    (0, (0, 1), (1, 0)),
    (0, (-1, 0), (-1, 0)),
    (0, (1, 0), (0, 1)),
    (1, (-1, 0), (1, 0)),
    (1, (1, 0), (0, 1)),
    (2, (-1, 0), (0, 1)),
    (4, (-1, 0), (0, 1)),
)


def come_from(routes, core):
    found = [(0, 0)]
    for source, *moves in routes:
        steps, cross = moves[core]
        at = found[source]
        found.append(((at[0] - steps) % 4, (at[1] + cross) % 2))
    return found


def tile_at(routes, core):
    found = come_from(routes, core)
    return [found.index((i % 4, i // 4)) for i in range(8)]


def send(array, ring, k):
    _, *moves = (Z_ROUTES if ring == "z" else X_ROUTES)[k]
    axes = ("yl", "z", "c") if ring == "z" else ("c", "x", "yh")
    pairs = []
    for c in range(2):
        steps, cross = moves[c]
        for i in range(4):
            for y in range(2):
                to_i, to_y = (i + steps) % 4, (y + cross) % 2
                if ring == "z":
                    pairs.append(((y * 4 + i) * 2 + c, (to_y * 4 + to_i) * 2 + c))
                else:
                    pairs.append(((c * 4 + i) * 2 + y, (c * 4 + to_i) * 2 + to_y))
    return lax.ppermute(array, axes, pairs)


def steps(
    potential, basis_left, basis_right, core_matrix, density, pattern, pair_atoms, cube_offsets,
    live_count,
):
    x, yh = lax.axis_index("x"), lax.axis_index("yh")
    yl, z, c = lax.axis_index("yl"), lax.axis_index("z"), lax.axis_index("c")

    offsets = cube_offsets.T
    prev_offsets = shift(offsets, ALL, 1)
    next_offsets = shift(offsets, ALL, -1)

    d = [density]
    for k in range(7):
        d.append(send(d[Z_ROUTES[k][0]], "z", k))

    for_prev, for_next = cut_edges(prev_offsets, next_offsets, potential)
    high = shift(for_prev, ALL, -1)
    low = shift(for_next, ALL, 1)
    own = cut_own(offsets, potential)
    outgoing = partial_blocks(
        pair_atoms.T, live_count, offsets, low, own, high, basis_left, basis_right
    )
    received = lax.all_to_all(outgoing, ALL, 0, 0, tiled=True)

    column = lax.axis_index(COL) * ATOM_COLS
    origins = jnp.where(
        c == 0, jnp.array(come_from(Z_ROUTES, 0)), jnp.array(come_from(Z_ROUTES, 1))
    )
    origin_rows = ((((yl + origins[:, 1]) & 1) * 4 + ((z + origins[:, 0]) & 3)) * 2 + c) * ATOM_ROWS

    def masked(tiles, first):
        return jnp.stack(
            [
                block_mask(
                    tile,
                    lax.dynamic_slice(
                        pattern, (origin_rows[first + k], column), (ATOM_ROWS, ATOM_COLS)
                    ),
                    NB,
                )
                for k, tile in enumerate(tiles)
            ]
        )

    early = masked(d[:4], 0)
    early_other = shift(early, "c", 1)

    corner = (lax.axis_index(ROW) * ATOM_ROWS, column)
    pattern_tile = lax.dynamic_slice(pattern, corner, (ATOM_ROWS, ATOM_COLS))
    hamiltonian = hamiltonian_tile(pattern_tile.reshape(-1), core_matrix, received)
    h = [hamiltonian]
    for k in range(7):
        h.append(send(h[X_ROUTES[k][0]], "x", k))

    late_tiles = lax.optimization_barrier((*d[4:], hamiltonian))[:4]
    late = masked(late_tiles, 4)
    late_other = shift(late, "c", 1)
    stacks = (early, late, early_other, late_other)

    sources = jnp.where(c == 0, jnp.array(come_from(X_ROUTES, 0)), jnp.array(come_from(X_ROUTES, 1)))
    block = ((x + sources[:, 0]) & 3) * 2 + ((yh + sources[:, 1]) & 1)
    at = (((block >> 2) + yl) & 1) * 4 + ((block - z) & 3)
    first, second = jnp.array(tile_at(Z_ROUTES, 0)), jnp.array(tile_at(Z_ROUTES, 1))
    hot = (at[:, None] == jnp.arange(8)[None, :]).astype(jnp.int32)
    in_own = jnp.sum(hot * jnp.where(c == 0, first, second)[None, :], axis=1)
    in_other = jnp.sum(hot * jnp.where(c == 0, second, first)[None, :], axis=1)
    index = jnp.concatenate([c.reshape(1), in_own, in_other]).astype(jnp.int32)

    out = multiply(index, 0, None, h[:3], stacks)
    out = multiply(index, 3, out, h[3:5], stacks)
    out = multiply(index, 5, out, h[5:7], stacks)
    out = multiply(index, 7, out, h[7:], stacks)
    return hamiltonian, out


def solution(mesh):
    split = Mesh(mesh.devices.reshape(2, 4, 2, 4, 2), ALL)
    placed = (
        P(ALL, None, None),
        P(ALL, None, None),
        P(ALL, None, None),
        P(ROW, COL),
        P(ROW, COL),
        P(),
        P(ALL, None),
        P(ALL, None),
        P(ALL),
    )
    return jax.shard_map(
        steps,
        mesh=split,
        in_specs=placed,
        out_specs=(P(ROW, COL), P(ROW, COL)),
        check_vma=False,
    )
```
